128 devices in a mesh: grp: 8 (over x, core), dev: 16 (over y, z).
Axes of the slice: x: 4, y: 4, z: 4, core: 2. Of those that a mesh axis runs over, the one named last changes fastest.
Arguments:
- sep_inv: bfloat16 [4096, 4096], P('grp', 'dev'), may hold values from -0.125 to 0.125
- panels: bfloat16 [8, 96, 2048, 128], P('grp', 'dev'), may hold values from -1.1953125 to 1.1953125
- diag_inverse: bfloat16 [8, 96, 768, 128], P('grp', 'dev'), may hold values from -6 to 6
- widths: int32 [8, 32], P('grp'), may hold values from 1 to 6, 96 in all within a row
- ancestors: int32 [8, 32, 16], P('grp'), may hold values from 0 to 31, as said below
Outputs:
- off_diag: bfloat16 [8, 96, 2048, 128], P('grp', 'dev')
- diag_panels: bfloat16 [8, 96, 768, 128], P('grp', 'dev')
The draws below stay inside these ranges and needn't reach their ends.
Inputs may be any that keep to these rules, and one draw needn't show every extreme that they name: `widths`: each row of a subtree sums to 96. `ancestors`: each supernode's list holds 16 different separator tile numbers in increasing order.
All inputs are finite; a program needn't handle non-finite values.
Results may differ from the reference program's by a relative error of at most 0.0046.
Values may be sent and summed in bfloat16 or wider, within the bound.
A program may use at most 320 MiB of HBM per device.

```python
import math
import jax
import jax.numpy as jnp
import numpy as np
from jax import lax

SEP = 4096
B = 128
ANC = 16
MAXU = 6
GROUPS = 8
UNITS = 96
NSG = 32
WMAX = 768


def draw_ancestors(key, part):
    count_blocks = SEP // B
    noise = jax.random.randint(key, (GROUPS, NSG, count_blocks), 0, 4 * count_blocks)
    index = jnp.arange(count_blocks, dtype=jnp.int32)
    scores = (noise + index) * count_blocks + index
    chosen = lax.top_k(scores, ANC)[1]
    return jnp.sort(chosen, axis=-1).astype(jnp.int32)


def block_levels(rng, shape, shards, low, high):
    def one(dim, parts):
        heights = jax.random.uniform(jax.random.fold_in(jax.random.fold_in(rng, 6), dim), (parts,), jnp.float32, low / len(shards), high / len(shards))
        return jnp.repeat(jnp.exp(heights), shape[dim] // parts).reshape((-1,) + (1,) * (len(shape) - dim - 1))

    loudness = one(*shards[0])
    for cut in shards[1:]:
        loudness = loudness * one(*cut)
    return loudness


def profile(count, total, reach, skew):
    weights = [(1 << 20) // math.isqrt(standing ** skew) + 1 for standing in range(2, count + 1)]
    spare, counts = total - reach - (count - 1), [1] * (count - 1)
    while spare > 0:
        candidates = [i for i in range(count - 1) if counts[i] < reach]
        whole, left = sum([weights[i] for i in candidates]), spare
        for i in candidates:
            more = min(reach - counts[i], max(1, left * weights[i] // whole), spare)
            counts[i] = counts[i] + more
            spare = spare - more
    return np.array([reach] + counts)


def uneven_parts(stream_key, count, total, limit, lean):
    if count == 2:
        one = jax.random.randint(stream_key, (), max(1, total - limit), min(limit, total - 1) + 1)
        return jnp.stack([one, total - one])
    sizes = jnp.asarray(profile(count, total, limit, lean), jnp.int32)
    couples = (count - 1) // 2
    giver, receiver = sizes[1:1 + 2 * couples:2], sizes[2:2 + 2 * couples:2]
    room = jnp.minimum(giver - 1, limit - receiver)
    passed = jax.random.randint(jax.random.fold_in(stream_key, 1), (couples,), 0, 1 << 20) % (room + 1)
    sizes = sizes.at[1:1 + 2 * couples:2].set(giver - passed).at[2:2 + 2 * couples:2].set(receiver + passed)
    return sizes[jax.random.permutation(jax.random.fold_in(stream_key, 2), count)]


def scatter_about(stream_key, dims, deviation, most, split=(), held_as=jnp.bfloat16):
    array = jax.random.normal(stream_key, dims, jnp.float32) * deviation
    if len(split) > 0:
        array = block_levels(stream_key, dims, split, -0.22, 0.18) * array
    return jnp.clip(array, min=-most, max=most).astype(held_as)


def setup_inputs(seed: int = 0) -> dict:
    seeds = jax.random.split(jax.random.key(seed), 6)
    return {
        "sep_inv": scatter_about(seeds[0], (SEP, SEP), (ANC * B) ** -0.5, 0.125, ((0, 8), (1, 16))),
        "panels": scatter_about(seeds[1], (GROUPS, UNITS, ANC * B, B), 0.2, 1.1953125, ((0, 8), (1, 16))),
        "diag_inverse": scatter_about(seeds[2], (GROUPS, UNITS, WMAX, B), 1.0, 6.0, ((0, 8), (1, 16))),
        "widths": jax.vmap(lambda own: uneven_parts(own, NSG, UNITS, MAXU, 1))(jax.random.split(seeds[3], GROUPS)).reshape((GROUPS, NSG)).astype(jnp.int32),
        "ancestors": draw_ancestors(jax.random.fold_in(seeds[5], 71), 0),
    }


def reference(sep_inv, panels, diag_inverse, widths, ancestors):
    units = panels.shape[1]
    count_blocks = SEP // B
    tiles = sep_inv.astype(jnp.float32).reshape(count_blocks, B, count_blocks, B).transpose(0, 2, 1, 3)

    def per_group(group_args):
        panel_g, dinv_g, width_g, anc_g = group_args
        ends = jnp.cumsum(width_g).astype(jnp.int32)
        starts = ends - width_g
        position = jnp.arange(units, dtype=jnp.int32)
        owner = jnp.sum((ends[None, :] <= position[:, None]).astype(jnp.int32), axis=1).astype(jnp.int32)
        column = position - starts[owner]
        width_u = width_g[owner]
        blocks = anc_g[owner]
        padded = jnp.pad(panel_g, ((MAXU - 1, MAXU - 1), (0, 0), (0, 0)))

        def per_unit(unit_idx):
            chosen = blocks[unit_idx]
            picked = tiles[chosen[:, None], chosen[None, :]]
            panel_u = panel_g[unit_idx].astype(jnp.float32).reshape(ANC, B, B)
            product = jnp.einsum('abij,bjc->aic', picked, panel_u).reshape(ANC * B, B)
            result_x = (-product).astype(jnp.bfloat16)
            start_at = (unit_idx + MAXU - 1 - column[unit_idx]).astype(jnp.int32)
            related = lax.dynamic_slice_in_dim(padded, start_at, MAXU, 0)
            inner = jnp.einsum('jrb,rc->jbc', related.astype(jnp.float32), result_x.astype(jnp.float32))
            keep = (jnp.arange(MAXU, dtype=jnp.int32) < width_u[unit_idx]).astype(jnp.float32)
            diag_block = (dinv_g[unit_idx].astype(jnp.float32).reshape(MAXU, B, B) - inner) * keep[:, None, None]
            return result_x, diag_block.reshape(MAXU * B, B).astype(jnp.bfloat16)

        return lax.map(per_unit, jnp.arange(units, dtype=jnp.int32))

    off_diag, diag_panels = lax.map(per_group, (panels, diag_inverse, widths, ancestors))
    return off_diag, diag_panels
```

```python
import functools
import heapq

import jax
import jax.numpy as jnp
from jax import lax
from jax.experimental import pallas as pl
from jax.experimental.pallas import tpu as pltpu
from jax.sharding import PartitionSpec as P

MESH = pl.DeviceIdType.MESH
F32 = jnp.float32
BF16 = jnp.bfloat16
ORDER = (("y", "z", "x"), ("z", "y", "x"), ("z", "x", "y"), ("y", "x", "z"))
B = 128
LOCAL = 6
EDGE = 5
ANC = 16
TILES = 32
NSG = 32
CHUNKS = 16
KC = 256
SPREADS = 4
HALOS = 20


def plan():
    rate, latency, piece, edge = 44e3, 2.2, B * KC * 2, 512 * B * 2
    steps, free, heap, got, tasks = [], {}, [], {}, []
    clock = 0.0
    cost = {"A": 1.4, "B": 2.1, "C": 2.1}

    def send(m):
        part, phase, _, s, kind = m
        link = (ORDER[part][phase - 1], s)
        size = piece * (4 if phase == 3 else 1) // (2 if kind == "half" else 1)
        free[link] = max(clock, free.get(link, 0.0)) + size / rate
        heapq.heappush(heap, (free[link] + latency, len(steps), m))
        steps.append(("send", m))

    def near(part, phase, a):
        for s in (1, -1):
            send((part, phase, a, s, "near"))

    def count(key):
        got[key] = got.get(key, 0) + 1
        return got[key]

    def plane(part, rel):
        if part < 2:
            if count(("A", rel)) == 8:
                tasks.extend(("A", rel, i) for i in range(3))
        elif count((part, "plane", rel)) == 4:
            tasks.append(("B" if part == 2 else "C", rel, count((part, "order"))))

    def handle(m):
        part, phase, a, s, kind = m
        if phase == 1:
            if kind == "near":
                send((part, 1, 0, s, "half"))
                near(part, 2, -s)
                full = count((part, 1))
            elif count((part, 1, "far")) == 2:
                near(part, 2, 2)
                full = count((part, 1))
            else:
                full = 0
            if full == 3:
                near(part, 3, 0)
                plane(part, 0)
        elif phase == 2:
            if kind == "near":
                send((part, 2, a, s, "half"))
                if count((part, 2, -s)) == 4:
                    near(part, 3, -s)
                    plane(part, 0)
            elif count((part, 2, 2)) == 8:
                near(part, 3, 2)
                plane(part, 0)
        elif kind == "near":
            send((part, 3, a, s, "half"))
            plane(part, -s)
        elif count((part, 3, a, "far")) == 2:
            plane(part, 2)

    for phase in (1, 2):
        for part in range(4):
            near(part, phase, 0)
    edges = 0
    while heap or tasks:
        while heap and heap[0][0] <= clock:
            m = heapq.heappop(heap)[2]
            steps.append(("wait", m))
            handle(m)
        while edges < HALOS and 8 < clock and free[("z", 1)] < clock + 4:
            for s in (1, -1):
                free[("z", s)] = max(clock, free[("z", s)]) + edge / rate
            steps.append(("edge", edges))
            edges += 1
        if tasks:
            task = tasks.pop(0)
            steps.append(("task",) + task)
            clock += cost[task[0]]
        elif heap:
            clock = max(clock, heap[0][0])
    return steps + [("edge", i) for i in range(edges, HALOS)]


def spans(widths, position):
    def step(k, carry):
        end, owner, start, width = carry
        w = widths[0, k]
        inside = [(position + u >= end) & (position + u < end + w) for u in range(LOCAL)]
        owner = tuple(jnp.where(i, k, o) for i, o in zip(inside, owner))
        start = tuple(jnp.where(i, end, o) for i, o in zip(inside, start))
        width = tuple(jnp.where(i, w, o) for i, o in zip(inside, width))
        return end + w, owner, start, width

    zeros = (jnp.int32(0),) * LOCAL
    _, owner, start, width = lax.fori_loop(0, NSG, step, (jnp.int32(0), zeros, zeros, zeros))
    return owner, start, width


def spread_kernel(widths, ancestors, panel, out, table, spot):
    u = pl.program_id(0)

    @pl.when(u == 0)
    def _():
        owner, start, width = spans(widths, lax.axis_index("dev") * LOCAL)
        for v in range(LOCAL):
            table[0, v] = owner[v]
            table[1, v] = lax.axis_index("dev") * LOCAL + v - start[v]
            table[2, v] = width[v]
            for t in range(TILES):
                spot[v, t] = ANC
        for v in range(LOCAL):
            for a in range(ANC):
                spot[v, ancestors[0, owner[v], a]] = a

    for t in range(TILES):
        a = spot[u, t]
        rows = pl.ds(pl.multiple_of(jnp.minimum(a, ANC - 1) * B, B), B)
        value = panel[0, 0, rows, :]
        out[t // 2, (t % 2) * B:(t % 2 + 1) * B, :] = jnp.where(a < ANC, value, jnp.zeros_like(value))


def gather_kernel(
    steps, sep, panels, spread, y_out, left_out, right_out,
    blocks, own, other, total, stage_own, stage_other,
    load_sem, own_sem, send_sem, recv_sem, half_send, half_recv, y_local, y_send, y_recv, edge_send, edge_recv,
):
    grp, dev = lax.axis_index("grp"), lax.axis_index("dev")
    core = lax.rem(grp, 2)
    at = {"x": grp // 2, "y": dev // 4, "z": lax.rem(dev, 4)}

    def moved(axis, by):
        return lax.rem(at[axis] + by + 4, 4)

    def device(axis, by):
        to = dict(at)
        to[axis] = moved(axis, by)
        return (to["x"] * 2 + core, to["y"] * 4 + to["z"])

    partner = (at["x"] * 2 + 1 - core, dev)
    ahead, behind = (grp, lax.rem(dev + 1, 16)), (grp, lax.rem(dev + 15, 16))

    loads = [
        pltpu.make_async_copy(
            sep.at[pl.ds(p * B, B)], blocks.at[p, at["x"], at["y"], at["z"]], load_sem.at[p]
        )
        for p in range(4)
    ]
    own_load = pltpu.make_async_copy(spread, own, own_sem)
    for c in loads:
        c.start()
    own_load.start()
    barrier = pltpu.get_barrier_semaphore()
    greeted = [device(a, s) for a in ("x", "y", "z") for s in (1, -1)] + [partner, ahead, behind]
    for d in greeted:
        pl.semaphore_signal(barrier, inc=1, device_id=d, device_id_type=MESH)
    for c in loads:
        c.wait()
    pl.semaphore_wait(barrier, len(greeted))

    number = {m: i for i, m in enumerate(s[1] for s in steps if s[0] == "send")}

    def message(m, arriving):
        part, phase, a, s, kind = m
        axes = ORDER[part]
        axis = axes[phase - 1]
        where = dict(at)
        if phase == 2:
            where[axes[0]] = moved(axes[0], a)
        if phase == 3:
            where[axes[0]] = slice(None)
            where[axes[1]] = moved(axes[1], a)
        gone = (0 if kind == "near" else 1) + (1 if arriving else 0)
        where[axis] = moved(axis, -s * gone)
        columns = slice(None) if kind == "near" else pl.ds(0 if s == 1 else B, B)
        ref = blocks.at[part, where["x"], where["y"], where["z"], slice(None), columns]
        if phase == 3:
            ref = blocks.at[part, where["x"], where["y"], where["z"], :, columns]
        return pltpu.make_async_remote_copy(
            src_ref=ref, dst_ref=ref, send_sem=send_sem.at[number[m]], recv_sem=recv_sem.at[number[m]],
            device_id=device(axis, s), device_id_type=MESH,
        )

    def spread_copy(i):
        some = pl.ds(CHUNKS // SPREADS * i, CHUNKS // SPREADS)
        return pltpu.make_async_remote_copy(
            src_ref=spread.at[some], dst_ref=other.at[some], send_sem=half_send.at[i], recv_sem=half_recv.at[i],
            device_id=partner, device_id_type=MESH,
        )

    def edge_copy(i):
        t, rows = i // 4, pl.ds((i % 4) * 512, 512)
        return [
            pltpu.make_async_remote_copy(
                src_ref=panels.at[0, LOCAL - EDGE + t, rows], dst_ref=left_out.at[t, rows],
                send_sem=edge_send.at[0], recv_sem=edge_recv.at[0], device_id=ahead, device_id_type=MESH,
            ),
            pltpu.make_async_remote_copy(
                src_ref=panels.at[0, t, rows], dst_ref=right_out.at[t, rows],
                send_sem=edge_send.at[1], recv_sem=edge_recv.at[1], device_id=behind, device_id_type=MESH,
            ),
        ]

    def results(i, x, tiles):
        here, there = pl.ds(tiles, 2 if tiles == 0 else 1), 2 * x + core
        return (
            pltpu.make_async_copy(stage_own.at[:, x, here], y_out.at[:, there, here], y_local.at[i]),
            pltpu.make_async_remote_copy(
                src_ref=stage_other.at[:, x, here], dst_ref=y_out.at[:, there, here],
                send_sem=y_send.at[i], recv_sem=y_recv.at[i], device_id=partner, device_id_type=MESH,
            ),
        )

    def arrived(i, x, tiles):
        here, there = pl.ds(tiles, 2 if tiles == 0 else 1), 2 * x + 1 - core
        return pltpu.make_async_remote_copy(
            src_ref=y_out.at[:, there, here], dst_ref=y_out.at[:, there, here],
            send_sem=y_send.at[i], recv_sem=y_recv.at[i], device_id=partner, device_id_type=MESH,
        )

    queued = []

    def put(x, tiles):
        i = len(queued)
        queued.append((i, x, tiles))
        for c in results(i, x, tiles):
            c.start()

    def task_a(rel, n):
        x = moved("x", rel)
        cols = pl.ds(n * 256, 256)
        for source, stage in ((own, stage_own), (other, stage_other)):
            acc = jnp.zeros((2 * B, 256), F32)
            for k in range(CHUNKS):
                lhs = blocks[0:2, x, k // 4, k % 4].reshape(2 * B, KC)
                acc = acc + jnp.dot(lhs, source[k, :, cols], preferred_element_type=F32)
            value = acc.astype(BF16)
            for p in range(2):
                for v in range(2):
                    stage[2 * n + v, x, p] = value[p * B:(p + 1) * B, v * B:(v + 1) * B]

    def task_bc(part, rel, nth):
        axis = "y" if part == 2 else "z"
        fixed = moved(axis, rel)
        for h, (source, stage) in enumerate(((own, stage_own), (other, stage_other))):
            def column(n, carry):
                acc = jnp.zeros((4 * B, 256), F32)
                cols = pl.ds(pl.multiple_of(n * 256, 256), 256)
                for k in range(4):
                    yy, zz = (fixed, k) if part == 2 else (k, fixed)
                    lhs = blocks[part, :, yy, zz].reshape(4 * B, KC)
                    acc = acc + jnp.dot(lhs, source[yy * 4 + zz, :, cols], preferred_element_type=F32)
                slot = (part - 2, 3 * h + n)
                if nth == 1:
                    total[slot] = acc
                elif nth < 4:
                    total[slot] = total[slot] + acc
                else:
                    value = (total[slot] + acc).astype(BF16)
                    for x in range(4):
                        for v in range(2):
                            stage[2 * n + v, x, part] = value[x * B:(x + 1) * B, v * B:(v + 1) * B]
                return carry

            lax.fori_loop(0, 3, column, 0)

    for j in range(SPREADS):
        spread_copy(j).start()
    got_other = False
    for step in steps:
        if step[0] == "send":
            message(step[1], False).start()
        elif step[0] == "wait":
            message(step[1], True).wait_recv()
        elif step[0] == "edge":
            for c in edge_copy(step[1]):
                c.start()
        else:
            _, name, rel, i = step
            if not got_other:
                own_load.wait()
                for j in range(SPREADS):
                    spread_copy(j).wait_recv()
                got_other = True
            if name == "A":
                task_a(rel, i)
                if i == 2:
                    put(moved("x", rel), 0)
            else:
                part = 2 if name == "B" else 3
                task_bc(part, rel, i)
                if i == 4:
                    for x in range(4):
                        put(x, part)

    for i, x, tiles in queued:
        arrived(i, x, tiles).wait_recv()
    for i, x, tiles in queued:
        local, remote = results(i, x, tiles)
        local.wait()
        remote.wait_send()
    for j in range(SPREADS):
        spread_copy(j).wait_send()
    for m in number:
        message(m, False).wait_send()
    for e, (out, d) in enumerate(((left_out, ahead), (right_out, behind))):
        whole = pltpu.make_async_remote_copy(
            src_ref=panels.at[0, pl.ds(0, EDGE)], dst_ref=out, send_sem=edge_send.at[e], recv_sem=edge_recv.at[e],
            device_id=d, device_id_type=MESH,
        )
        whole.wait_recv()
        whole.wait_send()


def finish_kernel(table, ancestors, y, left, mine, right, diag, off, out, ext, sem):
    u = pl.program_id(0)
    copies = [
        pltpu.make_async_copy(left, ext.at[pl.ds(0, EDGE)], sem.at[0]),
        pltpu.make_async_copy(mine.at[0], ext.at[pl.ds(EDGE, LOCAL)], sem.at[1]),
        pltpu.make_async_copy(right, ext.at[pl.ds(EDGE + LOCAL, EDGE)], sem.at[2]),
    ]

    @pl.when(u == 0)
    def _():
        for c in copies:
            c.start()

    for a in range(ANC):
        off[0, 0, a * B:(a + 1) * B] = -y[0, ancestors[0, table[0, u], a]]

    @pl.when(u == 0)
    def _():
        for c in copies:
            c.wait()

    x = off[0, 0]
    first = u + EDGE - table[1, u]
    for j in range(LOCAL):
        inner = lax.dot_general(ext[first + j], x, (((0,), (0,)), ((), ())), preferred_element_type=F32)
        rows = slice(j * B, (j + 1) * B)
        kept = jnp.where(j < table[2, u], diag[0, 0, rows].astype(F32) - inner, 0.0)
        out[0, 0, rows] = kept.astype(BF16)


def on_device(sep_inv, panels, diag_inverse, widths, ancestors):
    steps = plan()
    sends = sum(s[0] == "send" for s in steps)
    any_space = pl.BlockSpec(memory_space=pl.ANY)
    smem = pl.BlockSpec(memory_space=pltpu.SMEM)
    dma = pltpu.SemaphoreType.DMA
    spread, table = pl.pallas_call(
        spread_kernel,
        name="spread",
        grid=(LOCAL,),
        in_specs=[smem, smem, pl.BlockSpec((1, 1, ANC * B, B), lambda u: (0, u, 0, 0))],
        out_specs=(pl.BlockSpec((CHUNKS, KC, B), lambda u: (0, 0, u)), smem),
        out_shape=(
            jax.ShapeDtypeStruct((CHUNKS, KC, LOCAL * B), BF16),
            jax.ShapeDtypeStruct((3, LOCAL), jnp.int32),
        ),
        scratch_shapes=[pltpu.SMEM((LOCAL, TILES), jnp.int32)],
    )(widths, ancestors, panels)
    y, left, right = pl.pallas_call(
        functools.partial(gather_kernel, steps),
        name="gather",
        out_shape=(
            jax.ShapeDtypeStruct((LOCAL, 8, 4, B, B), BF16),
            jax.ShapeDtypeStruct((EDGE, ANC * B, B), BF16),
            jax.ShapeDtypeStruct((EDGE, ANC * B, B), BF16),
        ),
        in_specs=[any_space, any_space, any_space],
        out_specs=(any_space, any_space, any_space),
        scratch_shapes=[
            pltpu.VMEM((4, 4, 4, 4, B, KC), BF16),
            pltpu.VMEM((CHUNKS, KC, LOCAL * B), BF16),
            pltpu.VMEM((CHUNKS, KC, LOCAL * B), BF16),
            pltpu.VMEM((2, 6, 4 * B, 256), F32),
            pltpu.VMEM((LOCAL, 4, 4, B, B), BF16),
            pltpu.VMEM((LOCAL, 4, 4, B, B), BF16),
            dma((4,)),
            dma,
            dma((sends,)),
            dma((sends,)),
            dma((SPREADS,)),
            dma((SPREADS,)),
            dma((12,)),
            dma((12,)),
            dma((12,)),
            dma((2,)),
            dma((2,)),
        ],
        compiler_params=pltpu.CompilerParams(
            collective_id=0, has_side_effects=True, vmem_limit_bytes=60 * 1024 * 1024
        ),
    )(sep_inv, panels, spread)

    def unit(rows):
        return pl.BlockSpec((1, 1, rows, B), lambda u, *_: (0, u, 0, 0))

    off, diag = pl.pallas_call(
        finish_kernel,
        name="finish",
        grid_spec=pltpu.PrefetchScalarGridSpec(
            num_scalar_prefetch=2,
            grid=(LOCAL,),
            in_specs=[
                pl.BlockSpec((1, TILES, B, B), lambda u, *_: (u, 0, 0, 0)),
                any_space, any_space, any_space, unit(LOCAL * B),
            ],
            out_specs=[unit(ANC * B), unit(LOCAL * B)],
            scratch_shapes=[pltpu.VMEM((2 * EDGE + LOCAL, ANC * B, B), BF16), dma((3,))],
        ),
        out_shape=(
            jax.ShapeDtypeStruct((1, LOCAL, ANC * B, B), BF16),
            jax.ShapeDtypeStruct((1, LOCAL, LOCAL * B, B), BF16),
        ),
        compiler_params=pltpu.CompilerParams(vmem_limit_bytes=40 * 1024 * 1024),
    )(table, ancestors, y.reshape(LOCAL, TILES, B, B), left, panels, right, diag_inverse)
    return off, diag


def solution(mesh):
    placed = (
        P("grp", "dev"),
        P("grp", "dev", None, None),
        P("grp", "dev", None, None),
        P("grp", None),
        P("grp", None, None),
    )
    return jax.shard_map(
        on_device,
        mesh=mesh,
        in_specs=placed,
        out_specs=(P("grp", "dev", None, None), P("grp", "dev", None, None)),
        check_vma=False,
    )
```

```python
import functools
import heapq

import jax
import jax.numpy as jnp
from jax import lax
from jax.experimental import pallas as pl
from jax.experimental.pallas import tpu as pltpu
from jax.sharding import PartitionSpec as P

MESH = pl.DeviceIdType.MESH
F32 = jnp.float32
BF16 = jnp.bfloat16
PARTS = (
    (0, 0, 128, ("y", "z", "x")),
    (1, 0, 128, ("z", "y", "x")),
    (2, 0, 128, ("z", "x", "y")),
    (3, 0, 64, ("z", "x", "y")),
    (3, 64, 64, ("y", "x", "z")),
)
ORDER = tuple(p[3] for p in PARTS)
B = 128
LOCAL = 6
EDGE = 5
ANC = 16
TILES = 32
NSG = 32
CHUNKS = 16
KC = 256
SPREADS = 8
HALOS = 20


def plan():
    rate, latency, depth, edge = 42e3, 2.5, 4.0, 512 * B * 2
    steps, heap, got, held = [], [], {"edges": 0}, {2: [], 3: [], 4: []}
    queue = {(axis, s): [] for axis in ("x", "y", "z") for s in (1, -1)}
    free = {link: 0.0 for link in queue}
    tasks = [("spread", 0, i) for i in range(SPREADS)]
    clock = 0.0
    cost = {"spread": 0.5, "A": 1.25, "far": 0.95, "plane": 1.7, "group": 0.9}

    def send(m):
        part, phase, a, s, kind = m
        link = (ORDER[part][phase - 1], s)
        heapq.heappush(queue[link], (phase, kind == "half", len(steps), count("sent"), m))

    def pump():
        for link, waiting in queue.items():
            while waiting and free[link] < clock + depth:
                m = heapq.heappop(waiting)[4]
                size = PARTS[m[0]][2] * KC * 2 * (4 if m[1] == 3 else 1) // (2 if m[4] == "half" else 1)
                free[link] = max(clock, free[link]) + size / rate
                heapq.heappush(heap, (free[link] + latency, count("event"), m))
                steps.append(("send", m))
        while count("pump") and got["edges"] < HALOS and not queue["z", 1] and free["z", 1] < clock + depth:
            i = got["edges"]
            got["edges"] += 1
            for s in (1, -1):
                free["z", s] = max(clock, free["z", s]) + edge / rate
            steps.append(("edge", i))
            if i % 2:
                heapq.heappush(heap, (free["z", 1] + 2 * latency, count("event"), ("edge", i)))

    def near(part, phase, a):
        for s in (1, -1):
            send((part, phase, a, s, "near"))

    def count(key):
        got[key] = got.get(key, 0) + 1
        return got[key]

    def plane(part, rel):
        if part < 2:
            if count(("A", rel)) == 8:
                tasks.extend(("A", rel, i) for i in range(3))
        elif count((part, "plane", rel)) == 4:
            tasks.append(("plane", part, rel, count((part, "order"))))
            if got[(part, "order")] == 3:
                tasks.extend(held[part])

    def far(part, a):
        if part < 2:
            tasks.append(("far", part, a, count(("far", part))))
        else:
            group = ("group", part, a)
            (tasks if got.get((part, "order"), 0) == 3 else held[part]).append(group)

    def handle(m):
        part, phase, a, s, kind = m
        if phase == 1:
            if kind == "near":
                send((part, 1, 0, s, "half"))
                near(part, 2, -s)
                full = count((part, 1))
            elif count((part, 1, "far")) == 2:
                near(part, 2, 2)
                full = count((part, 1))
            else:
                full = 0
            if full == 3:
                near(part, 3, 0)
                plane(part, 0)
        elif phase == 2:
            if kind == "near":
                send((part, 2, a, s, "half"))
                if count((part, 2, -s)) == 4:
                    near(part, 3, -s)
                    plane(part, 0)
            elif count((part, 2, 2)) == 8:
                near(part, 3, 2)
                plane(part, 0)
        elif kind == "near":
            send((part, 3, a, s, "half"))
            plane(part, -s)
        elif count((part, 3, a, "far")) == 2:
            far(part, a)

    for phase in (1, 2):
        for part in range(len(PARTS)):
            near(part, phase, 0)
    pump()
    while heap or tasks or got["edges"] < HALOS:
        while heap and heap[0][0] <= clock:
            m = heapq.heappop(heap)[2]
            if m[0] == "edge":
                steps.append(("forward", m[1]))
                for s in (1, -1):
                    free["y", s] = max(clock, free["y", s]) + edge / rate
            else:
                steps.append(("wait", m))
                handle(m)
        pump()
        if tasks:
            task = tasks.pop(0)
            steps.append(("task",) + task)
            clock += cost[task[0]]
        elif heap:
            clock = max(clock, heap[0][0])
        else:
            clock += 1.0
    return steps


def spans(widths, position):
    def step(k, carry):
        end, owner, start, width = carry
        w = widths[0, k]
        inside = [(position + u >= end) & (position + u < end + w) for u in range(LOCAL)]
        owner = tuple(jnp.where(i, k, o) for i, o in zip(inside, owner))
        start = tuple(jnp.where(i, end, o) for i, o in zip(inside, start))
        width = tuple(jnp.where(i, w, o) for i, o in zip(inside, width))
        return end + w, owner, start, width

    zeros = (jnp.int32(0),) * LOCAL
    _, owner, start, width = lax.fori_loop(0, NSG, step, (jnp.int32(0), zeros, zeros, zeros))
    return owner, start, width


def table_kernel(widths, ancestors, table, spot):
    owner, start, width = spans(widths, lax.axis_index("dev") * LOCAL)
    for v in range(LOCAL):
        table[0, v] = owner[v]
        table[1, v] = lax.axis_index("dev") * LOCAL + v - start[v]
        table[2, v] = width[v]
        for t in range(TILES):
            spot[v, t] = ANC
        for a in range(ANC):
            spot[v, ancestors[0, owner[v], a]] = a


def gather_kernel(
    steps, sep, panels, spot, y_out, left_out, right_out, left_on, right_on,
    blocks, own, other, total, last, stage_own, stage_other, pan,
    load_sem, pan_sem, send_sem, recv_sem, half_send, half_recv, y_local, y_send, y_recv, edge_send, edge_recv,
    hop_send, hop_recv, on_send, on_recv,
):
    grp, dev = lax.axis_index("grp"), lax.axis_index("dev")
    core = lax.rem(grp, 2)
    at = {"x": grp // 2, "y": dev // 4, "z": lax.rem(dev, 4)}

    def moved(axis, by):
        return lax.rem(at[axis] + by + 4, 4)

    def device(axis, by):
        to = dict(at)
        to[axis] = moved(axis, by)
        return (to["x"] * 2 + core, to["y"] * 4 + to["z"])

    partner = (at["x"] * 2 + 1 - core, dev)
    ahead, behind = (grp, lax.rem(dev + 1, 16)), (grp, lax.rem(dev + 15, 16))

    loads = [
        pltpu.make_async_copy(
            sep.at[pl.ds(p * B, B)], blocks.at[p, at["x"], at["y"], at["z"]], load_sem.at[p]
        )
        for p in range(4)
    ]
    pan_load = pltpu.make_async_copy(panels.at[0], pan.at[:, pl.ds(0, ANC)], pan_sem)
    for c in loads:
        c.start()
    pan_load.start()
    pan[:, ANC] = jnp.zeros((LOCAL, B, B), BF16)
    barrier = pltpu.get_barrier_semaphore()
    greeted = [device(a, s) for a in ("x", "y", "z") for s in (1, -1)] + [partner, ahead, behind]
    for d in greeted:
        pl.semaphore_signal(barrier, inc=1, device_id=d, device_id_type=MESH)
    for c in loads:
        c.wait()
    pl.semaphore_wait(barrier, len(greeted))

    number = {m: i for i, m in enumerate(s[1] for s in steps if s[0] == "send")}

    def message(m, arriving):
        part, phase, a, s, kind = m
        axes = ORDER[part]
        axis = axes[phase - 1]
        row, low, rows, _ = PARTS[part]
        where = dict(at)
        if phase == 2:
            where[axes[0]] = moved(axes[0], a)
        if phase == 3:
            where[axes[0]] = slice(None)
            where[axes[1]] = moved(axes[1], a)
        gone = (0 if kind == "near" else 1) + (1 if arriving else 0)
        where[axis] = moved(axis, -s * gone)
        columns = slice(None) if kind == "near" else pl.ds(0 if s == 1 else B, B)
        ref = blocks.at[row, where["x"], where["y"], where["z"], pl.ds(low, rows), columns]
        return pltpu.make_async_remote_copy(
            src_ref=ref, dst_ref=ref, send_sem=send_sem.at[number[m]], recv_sem=recv_sem.at[number[m]],
            device_id=device(axis, s), device_id_type=MESH,
        )

    def spread_copy(i):
        some = pl.ds(CHUNKS // SPREADS * i, CHUNKS // SPREADS)
        return pltpu.make_async_remote_copy(
            src_ref=own.at[some], dst_ref=other.at[some], send_sem=half_send.at[i], recv_sem=half_recv.at[i],
            device_id=partner, device_id_type=MESH,
        )

    def edge_copy(i):
        t, rows = i // 4, pl.ds((i % 4) * 4, 4)
        sides = ((panels.at[0, LOCAL - EDGE + t, rows], left_out, ahead, 1), (panels.at[0, t, rows], right_out, behind, -1))
        return [
            pltpu.make_async_remote_copy(
                src_ref=src, dst_ref=out.at[t, rows],
                send_sem=hop_send.at[e, i // 2] if i % 2 else edge_send.at[e],
                recv_sem=hop_recv.at[e, i // 2] if i % 2 else edge_recv.at[e],
                device_id=device("z", s) if i % 2 else d, device_id_type=MESH,
            )
            for e, (src, out, d, s) in enumerate(sides)
        ]

    def edge_on(i):
        t, rows = i // 4, pl.ds((i % 4) * 4, 4)
        return [
            (at["z"] == z, pltpu.make_async_remote_copy(
                src_ref=out.at[t, rows], dst_ref=on.at[t, rows], send_sem=on_send.at[e, i // 2],
                recv_sem=on_recv.at[e, i // 2], device_id=device("y", s), device_id_type=MESH,
            ))
            for e, (out, on, z, s) in enumerate(((left_out, left_on, 0, 1), (right_out, right_on, 3, -1)))
        ]

    def results(i, x, tiles):
        here, there = pl.ds(tiles, 2 if tiles == 0 else 1), 2 * x + core
        return (
            pltpu.make_async_copy(stage_own.at[:, x, here], y_out.at[:, there, here], y_local.at[i]),
            pltpu.make_async_remote_copy(
                src_ref=stage_other.at[:, x, here], dst_ref=y_out.at[:, there, here],
                send_sem=y_send.at[i], recv_sem=y_recv.at[i], device_id=partner, device_id_type=MESH,
            ),
        )

    def arrived(i, x, tiles):
        here, there = pl.ds(tiles, 2 if tiles == 0 else 1), 2 * x + 1 - core
        return pltpu.make_async_remote_copy(
            src_ref=y_out.at[:, there, here], dst_ref=y_out.at[:, there, here],
            send_sem=y_send.at[i], recv_sem=y_recv.at[i], device_id=partner, device_id_type=MESH,
        )

    queued = []

    def put(x, tiles):
        i = len(queued)
        queued.append((i, x, tiles))
        for c in results(i, x, tiles):
            c.start()

    sides = ((own, stage_own), (other, stage_other))

    def keep(stage, n, x, part, value):
        row, low, rows, _ = part
        for v in range(2):
            stage[2 * n + v, x, row, low:low + rows] = value[:, v * B:(v + 1) * B]

    def task_a(rel, n):
        x = moved("x", rel)
        cols = pl.ds(n * 256, 256)
        for source, stage in sides:
            acc = jnp.zeros((2 * B, 256), F32)
            for k in range(CHUNKS):
                lhs = blocks[0:2, x, k // 4, k % 4].reshape(2 * B, KC)
                acc = acc + jnp.dot(lhs, source[k, :, cols], preferred_element_type=F32)
            value = acc.astype(BF16)
            for p in range(2):
                keep(stage, n, x, PARTS[p], value[p * B:(p + 1) * B])

    def columns(body):
        def column(n, carry):
            for h, (source, stage) in enumerate(sides):
                body(n, pl.ds(pl.multiple_of(n * 256, 256), 256), 3 * h + n, source, stage)
            return carry

        lax.fori_loop(0, 3, column, 0)

    def task_far(part, a, nth):
        x, fixed = moved("x", 2), moved(ORDER[part][1], a)

        def body(n, cols, slot, source, stage):
            acc = jnp.zeros((B, 256), F32)
            for k in range(4):
                y, z = (k, fixed) if part == 0 else (fixed, k)
                acc = acc + jnp.dot(blocks[part, x, y, z], source[y * 4 + z, :, cols], preferred_element_type=F32)
            if nth > 1:
                acc = acc + last[part, slot]
            if nth < 4:
                last[part, slot] = acc
            else:
                keep(stage, n, x, PARTS[part], acc.astype(BF16))

        columns(body)

    def tile_of(part, fixed, k):
        return (fixed, k) if ORDER[part][2] == "y" else (k, fixed)

    def some(part):
        row, low, rows, _ = PARTS[part]
        return row, pl.ds(low, rows), rows

    def task_plane(part, rel, nth):
        row, span, rows = some(part)
        fixed = moved(ORDER[part][2], rel)

        def body(n, cols, slot, source, stage):
            acc = jnp.zeros((4 * rows, 256), F32)
            for k in range(4):
                y, z = tile_of(part, fixed, k)
                lhs = blocks[row, :, y, z, span].reshape(4 * rows, KC)
                acc = acc + jnp.dot(lhs, source[y * 4 + z, :, cols], preferred_element_type=F32)
            if nth > 1:
                acc = acc + total[row - 2, slot, :, span].reshape(4 * rows, 256)
            total[row - 2, slot, :, span] = acc.reshape(4, rows, 256)

        columns(body)

    def task_group(part, a):
        row, span, rows = some(part)
        fixed, x = moved(ORDER[part][2], 2), moved("x", a)

        def body(n, cols, slot, source, stage):
            acc = total[row - 2, slot, x, span]
            for k in range(4):
                y, z = tile_of(part, fixed, k)
                acc = acc + jnp.dot(blocks[row, x, y, z, span], source[y * 4 + z, :, cols], preferred_element_type=F32)
            keep(stage, n, x, PARTS[part], acc.astype(BF16))

        columns(body)

    def spread(i):
        for j in range(4):
            t = 4 * i + j
            for u in range(LOCAL):
                own[t // 2, (t % 2) * B:(t % 2 + 1) * B, u * B:(u + 1) * B] = pan[u, spot[u, t]]

    got_other, ended = False, {}
    for step in steps:
        if step[0] == "send":
            message(step[1], False).start()
        elif step[0] == "wait":
            message(step[1], True).wait_recv()
        elif step[0] == "edge":
            for c in edge_copy(step[1]):
                c.start()
        elif step[0] == "forward":
            for c in edge_copy(step[1]):
                c.wait_recv()
            for c_if, c in edge_on(step[1]):
                pl.when(c_if)(c.start)
        else:
            name = step[1]
            if name == "spread":
                i = step[3]
                if i == 0:
                    pan_load.wait()
                spread(i)
                if i > 0:
                    spread_copy(i - 1).start()
                continue
            if not got_other:
                spread_copy(SPREADS - 1).start()
                for j in range(SPREADS):
                    spread_copy(j).wait_recv()
                got_other = True
            if name == "A":
                task_a(step[2], step[3])
                if step[3] == 2:
                    put(moved("x", step[2]), 0)
            elif name == "far":
                task_far(*step[2:])
                ended["far"] = ended.get("far", 0) + 1
                if ended["far"] == 8:
                    put(moved("x", 2), 0)
            elif name == "plane":
                task_plane(*step[2:])
            else:
                task_group(*step[2:])
                key = (PARTS[step[2]][0], step[3])
                ended[key] = ended.get(key, 0) + PARTS[step[2]][2]
                if ended[key] == B:
                    put(moved("x", step[3]), key[0])

    for i, x, tiles in queued:
        arrived(i, x, tiles).wait_recv()
    for i, x, tiles in queued:
        local, remote = results(i, x, tiles)
        local.wait()
        remote.wait_send()
    for j in range(SPREADS):
        spread_copy(j).wait_send()
    for m in number:
        message(m, False).wait_send()
    for i in range(1, HALOS, 2):
        for c in edge_copy(i):
            c.wait_send()
        for c_if, c in edge_on(i):
            pl.when(c_if)(c.wait)
    for e, (out, d) in enumerate(((left_out, ahead), (right_out, behind))):
        whole = pltpu.make_async_remote_copy(
            src_ref=panels.at[0, pl.ds(0, EDGE), pl.ds(0, ANC // 2)], dst_ref=out.at[:, pl.ds(0, ANC // 2)],
            send_sem=edge_send.at[e], recv_sem=edge_recv.at[e], device_id=d, device_id_type=MESH,
        )
        whole.wait_recv()
        whole.wait_send()


def finish_kernel(table, ancestors, y, left, mine, right, left_on, right_on, diag, off, out, ext, rows, ext_sem, row_sem):
    u = pl.program_id(0)
    z = lax.rem(lax.axis_index("dev"), 4)

    def pieces(source, first, e):
        return [
            pltpu.make_async_copy(
                source.at[:, pl.ds(4 * q, 4)], ext.at[pl.ds(first, EDGE), pl.ds(4 * q, 4)], ext_sem.at[e, q]
            )
            for q in range(4)
        ]

    middle = pltpu.make_async_copy(mine.at[0], ext.at[pl.ds(EDGE, LOCAL)], ext_sem.at[2, 0])
    edges = [
        (pieces(left, 0, 0), pieces(left_on, 0, 0), z == 0),
        (pieces(right, EDGE + LOCAL, 1), pieces(right_on, EDGE + LOCAL, 1), z == 3),
    ]

    row_copies = [pltpu.make_async_copy(y.at[v], rows.at[v], row_sem.at[v]) for v in range(LOCAL)]

    @pl.when(u == 0)
    def _():
        row_copies[0].start()
        middle.start()
        for near, far, crossed in edges:
            for q in range(4):
                if q % 2:
                    pl.when(crossed)(far[q].start)
                    pl.when(jnp.logical_not(crossed))(near[q].start)
                else:
                    near[q].start()
        for c in row_copies[1:]:
            c.start()

    pltpu.make_async_copy(y.at[u], rows.at[u], row_sem.at[u]).wait()
    for a in range(ANC):
        off[0, 0, a * B:(a + 1) * B] = -rows[u, ancestors[0, table[0, u], a]]
    x = off[0, 0].T

    @pl.when(u == 0)
    def _():
        middle.wait()
        for near, _, _ in edges:
            for c in near:
                c.wait()

    first = u + EDGE - table[1, u]
    for j in range(0, LOCAL, 2):
        pair = jnp.concatenate([ext[first + j].reshape(ANC * B, B), ext[first + j + 1].reshape(ANC * B, B)], axis=1)
        inner = jnp.dot(x, pair, preferred_element_type=F32)
        for v in range(2):
            at = slice((j + v) * B, (j + v + 1) * B)
            kept = diag[0, 0, at].astype(F32) - inner[:, v * B:(v + 1) * B].T
            out[0, 0, at] = jnp.where(j + v < table[2, u], kept, 0.0).astype(BF16)


def on_device(sep_inv, panels, diag_inverse, widths, ancestors):
    steps = plan()
    sends = sum(s[0] == "send" for s in steps)
    any_space = pl.BlockSpec(memory_space=pl.ANY)
    smem = pl.BlockSpec(memory_space=pltpu.SMEM)
    dma = pltpu.SemaphoreType.DMA
    hbm = pl.BlockSpec(memory_space=pltpu.HBM)
    tiled = panels.reshape(1, LOCAL, ANC, B, B)
    table, spot = pl.pallas_call(
        table_kernel,
        name="table",
        in_specs=[smem, smem],
        out_specs=(smem, smem),
        out_shape=(jax.ShapeDtypeStruct((3, LOCAL), jnp.int32), jax.ShapeDtypeStruct((LOCAL, TILES), jnp.int32)),
    )(widths, ancestors)
    y, left, right, left_on, right_on = pl.pallas_call(
        functools.partial(gather_kernel, steps),
        name="gather",
        out_shape=(
            jax.ShapeDtypeStruct((LOCAL, 8, 4, B, B), BF16),
        ) + (jax.ShapeDtypeStruct((EDGE, ANC, B, B), BF16),) * 4,
        in_specs=[any_space, any_space, smem],
        out_specs=(hbm,) * 5,
        scratch_shapes=[
            pltpu.VMEM((4, 4, 4, 4, B, KC), BF16),
            pltpu.VMEM((CHUNKS, KC, LOCAL * B), BF16),
            pltpu.VMEM((CHUNKS, KC, LOCAL * B), BF16),
            pltpu.VMEM((2, 6, 4, B, 256), F32),
            pltpu.VMEM((2, 6, B, 256), F32),
            pltpu.VMEM((LOCAL, 4, 4, B, B), BF16),
            pltpu.VMEM((LOCAL, 4, 4, B, B), BF16),
            pltpu.VMEM((LOCAL, ANC + 1, B, B), BF16),
            dma((4,)),
            dma,
            dma((sends,)),
            dma((sends,)),
            dma((SPREADS,)),
            dma((SPREADS,)),
            dma((12,)),
            dma((12,)),
            dma((12,)),
            dma((2,)),
            dma((2,)),
            dma((2, HALOS // 2)),
            dma((2, HALOS // 2)),
            dma((2, HALOS // 2)),
            dma((2, HALOS // 2)),
        ],
        compiler_params=pltpu.CompilerParams(
            collective_id=0, has_side_effects=True, vmem_limit_bytes=60 * 1024 * 1024
        ),
    )(sep_inv, tiled, spot)

    def unit(rows):
        return pl.BlockSpec((1, 1, rows, B), lambda u, *_: (0, u, 0, 0))

    off, diag = pl.pallas_call(
        finish_kernel,
        name="finish",
        grid_spec=pltpu.PrefetchScalarGridSpec(
            num_scalar_prefetch=2,
            grid=(LOCAL,),
            in_specs=[
                hbm, hbm, hbm, hbm, hbm, hbm, unit(LOCAL * B),
            ],
            out_specs=[unit(ANC * B), unit(LOCAL * B)],
            scratch_shapes=[
                pltpu.VMEM((2 * EDGE + LOCAL, ANC, B, B), BF16),
                pltpu.VMEM((LOCAL, TILES, B, B), BF16),
                dma((3, 4)),
                dma((LOCAL,)),
            ],
        ),
        out_shape=(
            jax.ShapeDtypeStruct((1, LOCAL, ANC * B, B), BF16),
            jax.ShapeDtypeStruct((1, LOCAL, LOCAL * B, B), BF16),
        ),
        compiler_params=pltpu.CompilerParams(vmem_limit_bytes=62 * 1024 * 1024),
    )(table, ancestors, y.reshape(LOCAL, TILES, B, B), left, tiled, right, left_on, right_on, diag_inverse)
    return off, diag


def solution(mesh):
    placed = (
        P("grp", "dev"),
        P("grp", "dev", None, None),
        P("grp", "dev", None, None),
        P("grp", None),
        P("grp", None, None),
    )
    return jax.shard_map(
        on_device,
        mesh=mesh,
        in_specs=placed,
        out_specs=(P("grp", "dev", None, None), P("grp", "dev", None, None)),
        check_vma=False,
    )
```

```python
import functools
import heapq

import jax
import jax.numpy as jnp
from jax import lax
from jax.experimental import pallas as pl
from jax.experimental.pallas import tpu as pltpu
from jax.sharding import PartitionSpec as P

MESH = pl.DeviceIdType.MESH
F32 = jnp.float32
BF16 = jnp.bfloat16
PARTS = (
    (0, 0, 128, ("y", "z", "x")),
    (1, 0, 128, ("z", "y", "x")),
    (2, 0, 128, ("z", "x", "y")),
    (3, 0, 64, ("z", "x", "y")),
    (3, 64, 64, ("y", "x", "z")),
)
ORDER = tuple(p[3] for p in PARTS)
B = 128
LOCAL = 6
EDGE = 5
ANC = 16
TILES = 32
NSG = 32
CHUNKS = 16
KC = 256
SPREADS = 8
HALOS = 20


def plan():
    rate, latency, depth, edge = 42e3, 2.5, 4.0, 512 * B * 2
    steps, heap, got, held = [], [], {"edges": 0}, {2: [], 3: [], 4: []}
    queue = {(axis, s): [] for axis in ("x", "y", "z") for s in (1, -1)}
    free = {link: 0.0 for link in queue}
    tasks = [("spread", 0, i) for i in range(SPREADS)]
    clock = 0.0
    cost = {"spread": 0.5, "A": 1.25, "far": 0.95, "plane": 1.7, "group": 0.9}

    def send(m):
        part, phase, a, s, kind = m
        link = (ORDER[part][phase - 1], s)
        heapq.heappush(queue[link], (phase, kind == "half", len(steps), count("sent"), m))

    def pump():
        for link, waiting in queue.items():
            while waiting and free[link] < clock + depth:
                m = heapq.heappop(waiting)[4]
                size = PARTS[m[0]][2] * KC * 2 * (4 if m[1] == 3 else 1) // (2 if m[4] == "half" else 1)
                free[link] = max(clock, free[link]) + size / rate
                heapq.heappush(heap, (free[link] + latency, count("event"), m))
                steps.append(("send", m))
        while count("pump") and got["edges"] < HALOS and not queue["z", 1] and free["z", 1] < clock + depth:
            i = got["edges"]
            got["edges"] += 1
            for s in (1, -1):
                free["z", s] = max(clock, free["z", s]) + edge / rate
            steps.append(("edge", i))
            if i % 2:
                heapq.heappush(heap, (free["z", 1] + 2 * latency, count("event"), ("edge", i)))

    def near(part, phase, a):
        for s in (1, -1):
            send((part, phase, a, s, "near"))

    def count(key):
        got[key] = got.get(key, 0) + 1
        return got[key]

    def plane(part, rel):
        if part < 2:
            if count(("A", rel)) == 8:
                tasks.extend(("A", rel, i) for i in range(3))
        elif count((part, "plane", rel)) == 4:
            tasks.append(("plane", part, rel, count((part, "order"))))
            if got[(part, "order")] == 3:
                tasks.extend(held[part])

    def far(part, a):
        if part < 2:
            tasks.append(("far", part, a, count(("far", part))))
        else:
            group = ("group", part, a)
            (tasks if got.get((part, "order"), 0) == 3 else held[part]).append(group)

    def handle(m):
        part, phase, a, s, kind = m
        if phase == 1:
            if kind == "near":
                send((part, 1, 0, s, "half"))
                near(part, 2, -s)
                full = count((part, 1))
            elif count((part, 1, "far")) == 2:
                near(part, 2, 2)
                full = count((part, 1))
            else:
                full = 0
            if full == 3:
                near(part, 3, 0)
                plane(part, 0)
        elif phase == 2:
            if kind == "near":
                send((part, 2, a, s, "half"))
                if count((part, 2, -s)) == 4:
                    near(part, 3, -s)
                    plane(part, 0)
            elif count((part, 2, 2)) == 8:
                near(part, 3, 2)
                plane(part, 0)
        elif kind == "near":
            send((part, 3, a, s, "half"))
            plane(part, -s)
        elif count((part, 3, a, "far")) == 2:
            far(part, a)

    for phase in (1, 2):
        for part in range(len(PARTS)):
            near(part, phase, 0)
    pump()
    while heap or tasks or got["edges"] < HALOS:
        while heap and heap[0][0] <= clock:
            m = heapq.heappop(heap)[2]
            if m[0] == "edge":
                steps.append(("forward", m[1]))
                for s in (1, -1):
                    free["y", s] = max(clock, free["y", s]) + edge / rate
            else:
                steps.append(("wait", m))
                handle(m)
        pump()
        if tasks:
            task = tasks.pop(0)
            steps.append(("task",) + task)
            clock += cost[task[0]]
        elif heap:
            clock = max(clock, heap[0][0])
        else:
            clock += 1.0
    return steps


def spans(widths, position, table):
    def step(k, end):
        w = widths[0, k]

        @pl.when((end < position + LOCAL) & (end + w > position))
        def _():
            for u in range(LOCAL):
                @pl.when((position + u >= end) & (position + u < end + w))
                def _():
                    table[0, u] = k
                    table[1, u] = position + u - end
                    table[2, u] = w

        return end + w

    lax.fori_loop(0, NSG, step, jnp.int32(0))


def table_kernel(widths, ancestors, table, spot):
    spans(widths, lax.axis_index("dev") * LOCAL, table)
    for v in range(LOCAL):
        owner = table[0, v]
        for t in range(TILES):
            spot[v, t] = ANC
        for a in range(ANC):
            spot[v, ancestors[0, a, owner]] = a


def gather_kernel(
    steps, sep, panels, spot, y_out, left_out, right_out, left_on, right_on,
    blocks, own, other, total, last, stage_own, stage_other, pan,
    load_sem, pan_sem, send_sem, recv_sem, half_send, half_recv, y_local, y_send, y_recv, edge_send, edge_recv,
    hop_send, hop_recv, on_send, on_recv,
):
    grp, dev = lax.axis_index("grp"), lax.axis_index("dev")
    core = lax.rem(grp, 2)
    at = {"x": grp // 2, "y": dev // 4, "z": lax.rem(dev, 4)}

    def moved(axis, by):
        return lax.rem(at[axis] + by + 4, 4)

    def device(axis, by):
        to = dict(at)
        to[axis] = moved(axis, by)
        return (to["x"] * 2 + core, to["y"] * 4 + to["z"])

    partner = (at["x"] * 2 + 1 - core, dev)
    ahead, behind = (grp, lax.rem(dev + 1, 16)), (grp, lax.rem(dev + 15, 16))

    loads = [
        pltpu.make_async_copy(
            sep.at[pl.ds(p * B, B)], blocks.at[p, at["x"], at["y"], at["z"]], load_sem.at[p]
        )
        for p in range(4)
    ]
    pan_load = pltpu.make_async_copy(panels.at[0], pan.at[:, pl.ds(0, ANC)], pan_sem)
    for c in loads:
        c.start()
    pan_load.start()
    pan[:, ANC] = jnp.zeros((LOCAL, B, B), BF16)
    barrier = pltpu.get_barrier_semaphore()
    greeted = [device(a, s) for a in ("x", "y", "z") for s in (1, -1)] + [partner, ahead, behind]
    for d in greeted:
        pl.semaphore_signal(barrier, inc=1, device_id=d, device_id_type=MESH)
    for c in loads:
        c.wait()
    pl.semaphore_wait(barrier, len(greeted))

    number = {m: i for i, m in enumerate(s[1] for s in steps if s[0] == "send")}

    def message(m, arriving):
        part, phase, a, s, kind = m
        axes = ORDER[part]
        axis = axes[phase - 1]
        row, low, rows, _ = PARTS[part]
        where = dict(at)
        if phase == 2:
            where[axes[0]] = moved(axes[0], a)
        if phase == 3:
            where[axes[0]] = slice(None)
            where[axes[1]] = moved(axes[1], a)
        gone = (0 if kind == "near" else 1) + (1 if arriving else 0)
        where[axis] = moved(axis, -s * gone)
        columns = slice(None) if kind == "near" else pl.ds(0 if s == 1 else B, B)
        ref = blocks.at[row, where["x"], where["y"], where["z"], pl.ds(low, rows), columns]
        return pltpu.make_async_remote_copy(
            src_ref=ref, dst_ref=ref, send_sem=send_sem.at[number[m]], recv_sem=recv_sem.at[number[m]],
            device_id=device(axis, s), device_id_type=MESH,
        )

    def spread_copy(i):
        some = pl.ds(CHUNKS // SPREADS * i, CHUNKS // SPREADS)
        return pltpu.make_async_remote_copy(
            src_ref=own.at[some], dst_ref=other.at[some], send_sem=half_send.at[i], recv_sem=half_recv.at[i],
            device_id=partner, device_id_type=MESH,
        )

    def edge_copy(i):
        t, rows = i // 4, pl.ds((i % 4) * 4, 4)
        sides = ((panels.at[0, LOCAL - EDGE + t, rows], left_out, ahead, 1), (panels.at[0, t, rows], right_out, behind, -1))
        return [
            pltpu.make_async_remote_copy(
                src_ref=src, dst_ref=out.at[t, rows],
                send_sem=hop_send.at[e, i // 2] if i % 2 else edge_send.at[e],
                recv_sem=hop_recv.at[e, i // 2] if i % 2 else edge_recv.at[e],
                device_id=device("z", s) if i % 2 else d, device_id_type=MESH,
            )
            for e, (src, out, d, s) in enumerate(sides)
        ]

    def edge_on(i):
        t, rows = i // 4, pl.ds((i % 4) * 4, 4)
        return [
            pltpu.make_async_remote_copy(
                src_ref=out.at[t, rows], dst_ref=on.at[t, rows], send_sem=on_send.at[e, i // 2],
                recv_sem=on_recv.at[e, i // 2], device_id=device("y", s), device_id_type=MESH,
            )
            for e, (out, on, s) in enumerate(((left_out, left_on, 1), (right_out, right_on, -1)))
        ]

    last_dev = 15
    sends_edge, takes_edge = (dev < last_dev, dev > 0), (dev > 0, dev < last_dev)
    first_z, last_z = at["z"] == 0, at["z"] == 3
    sends_on = (first_z & (at["y"] < 3), last_z & (at["y"] > 0))
    takes_on = (first_z & (at["y"] > 0), last_z & (at["y"] < 3))

    def results(i, x, tiles):
        here, there = pl.ds(tiles, 2 if tiles == 0 else 1), 2 * x + core
        return (
            pltpu.make_async_copy(stage_own.at[:, x, here], y_out.at[:, there, here], y_local.at[i]),
            pltpu.make_async_remote_copy(
                src_ref=stage_other.at[:, x, here], dst_ref=y_out.at[:, there, here],
                send_sem=y_send.at[i], recv_sem=y_recv.at[i], device_id=partner, device_id_type=MESH,
            ),
        )

    def arrived(i, x, tiles):
        here, there = pl.ds(tiles, 2 if tiles == 0 else 1), 2 * x + 1 - core
        return pltpu.make_async_remote_copy(
            src_ref=y_out.at[:, there, here], dst_ref=y_out.at[:, there, here],
            send_sem=y_send.at[i], recv_sem=y_recv.at[i], device_id=partner, device_id_type=MESH,
        )

    queued = []

    def put(x, tiles):
        i = len(queued)
        queued.append((i, x, tiles))
        for c in results(i, x, tiles):
            c.start()

    sides = ((own, stage_own), (other, stage_other))

    def keep(stage, n, x, part, value):
        row, low, rows, _ = part
        for v in range(2):
            stage[2 * n + v, x, row, low:low + rows] = value[:, v * B:(v + 1) * B]

    def task_a(rel, n):
        x = moved("x", rel)
        cols = pl.ds(n * 256, 256)
        for source, stage in sides:
            acc = jnp.zeros((2 * B, 256), F32)
            for k in range(CHUNKS):
                lhs = blocks[0:2, x, k // 4, k % 4].reshape(2 * B, KC)
                acc = acc + jnp.dot(lhs, source[k, :, cols], preferred_element_type=F32)
            value = acc.astype(BF16)
            for p in range(2):
                keep(stage, n, x, PARTS[p], value[p * B:(p + 1) * B])

    def columns(body):
        def column(n, carry):
            for h, (source, stage) in enumerate(sides):
                body(n, pl.ds(pl.multiple_of(n * 256, 256), 256), 3 * h + n, source, stage)
            return carry

        lax.fori_loop(0, 3, column, 0)

    def task_far(part, a, nth):
        x, fixed = moved("x", 2), moved(ORDER[part][1], a)

        def body(n, cols, slot, source, stage):
            acc = jnp.zeros((B, 256), F32)
            for k in range(4):
                y, z = (k, fixed) if part == 0 else (fixed, k)
                acc = acc + jnp.dot(blocks[part, x, y, z], source[y * 4 + z, :, cols], preferred_element_type=F32)
            if nth > 1:
                acc = acc + last[part, slot]
            if nth < 4:
                last[part, slot] = acc
            else:
                keep(stage, n, x, PARTS[part], acc.astype(BF16))

        columns(body)

    def tile_of(part, fixed, k):
        return (fixed, k) if ORDER[part][2] == "y" else (k, fixed)

    def some(part):
        row, low, rows, _ = PARTS[part]
        return row, pl.ds(low, rows), rows

    def task_plane(part, rel, nth):
        row, span, rows = some(part)
        fixed = moved(ORDER[part][2], rel)

        def body(n, cols, slot, source, stage):
            acc = jnp.zeros((4 * rows, 256), F32)
            for k in range(4):
                y, z = tile_of(part, fixed, k)
                lhs = blocks[row, :, y, z, span].reshape(4 * rows, KC)
                acc = acc + jnp.dot(lhs, source[y * 4 + z, :, cols], preferred_element_type=F32)
            if nth > 1:
                acc = acc + total[row - 2, slot, :, span].reshape(4 * rows, 256)
            total[row - 2, slot, :, span] = acc.reshape(4, rows, 256)

        columns(body)

    def task_group(part, a):
        row, span, rows = some(part)
        fixed, x = moved(ORDER[part][2], 2), moved("x", a)

        def body(n, cols, slot, source, stage):
            acc = total[row - 2, slot, x, span]
            for k in range(4):
                y, z = tile_of(part, fixed, k)
                acc = acc + jnp.dot(blocks[row, x, y, z, span], source[y * 4 + z, :, cols], preferred_element_type=F32)
            keep(stage, n, x, PARTS[part], acc.astype(BF16))

        columns(body)

    def spread(i):
        for j in range(4):
            t = 4 * i + j
            for u in range(LOCAL):
                own[t // 2, (t % 2) * B:(t % 2 + 1) * B, u * B:(u + 1) * B] = pan[u, spot[u, t]]

    got_other, ended = False, {}
    for step in steps:
        if step[0] == "send":
            message(step[1], False).start()
        elif step[0] == "wait":
            message(step[1], True).wait_recv()
        elif step[0] == "edge":
            for c, sends in zip(edge_copy(step[1]), sends_edge):
                if step[1] % 2:
                    c.start()
                else:
                    pl.when(sends)(c.start)
        elif step[0] == "forward":
            for c in edge_copy(step[1]):
                c.wait_recv()
            for c, sends in zip(edge_on(step[1]), sends_on):
                pl.when(sends)(c.start)
        else:
            name = step[1]
            if name == "spread":
                i = step[3]
                if i == 0:
                    pan_load.wait()
                spread(i)
                if i > 0:
                    spread_copy(i - 1).start()
                continue
            if not got_other:
                spread_copy(SPREADS - 1).start()
                for j in range(SPREADS):
                    spread_copy(j).wait_recv()
                got_other = True
            if name == "A":
                task_a(step[2], step[3])
                if step[3] == 2:
                    put(moved("x", step[2]), 0)
            elif name == "far":
                task_far(*step[2:])
                ended["far"] = ended.get("far", 0) + 1
                if ended["far"] == 8:
                    put(moved("x", 2), 0)
            elif name == "plane":
                task_plane(*step[2:])
            else:
                task_group(*step[2:])
                key = (PARTS[step[2]][0], step[3])
                ended[key] = ended.get(key, 0) + PARTS[step[2]][2]
                if ended[key] == B:
                    put(moved("x", step[3]), key[0])

    for i, x, tiles in queued:
        arrived(i, x, tiles).wait_recv()
    for i, x, tiles in queued:
        local, remote = results(i, x, tiles)
        local.wait()
        remote.wait_send()
    for j in range(SPREADS):
        spread_copy(j).wait_send()
    for m in number:
        message(m, False).wait_send()
    for i in range(1, HALOS, 2):
        for c in edge_copy(i):
            c.wait_send()
        for c, sends, takes in zip(edge_on(i), sends_on, takes_on):
            pl.when(sends)(c.wait_send)
            pl.when(takes)(c.wait_recv)
    for e, (out, d) in enumerate(((left_out, ahead), (right_out, behind))):
        whole = pltpu.make_async_remote_copy(
            src_ref=panels.at[0, pl.ds(0, EDGE), pl.ds(0, ANC // 2)], dst_ref=out.at[:, pl.ds(0, ANC // 2)],
            send_sem=edge_send.at[e], recv_sem=edge_recv.at[e], device_id=d, device_id_type=MESH,
        )
        pl.when(takes_edge[e])(whole.wait_recv)
        pl.when(sends_edge[e])(whole.wait_send)


def finish_kernel(table, ancestors, y, left, mine, right, left_on, right_on, diag, off, out, ext, rows, ext_sem, row_sem):
    u = pl.program_id(0)
    z = lax.rem(lax.axis_index("dev"), 4)
    before, after = table[1, 0], table[2, LOCAL - 1] - 1 - table[1, LOCAL - 1]

    def row_copies(v, wait):
        if wait:
            pltpu.make_async_copy(y.at[v, pl.ds(0, ANC)], rows.at[v], row_sem.at[v]).wait()
        else:
            for a in range(ANC):
                pltpu.make_async_copy(
                    y.at[v, ancestors[0, a, table[0, v]]], rows.at[v, a], row_sem.at[v]
                ).start()

    def tile_copies(t, wait):
        def copy(source, at, parts):
            for q in range(0, ANC, ANC // parts):
                span = pl.ds(q, ANC // parts)
                ref = source[q // 4 % 2] if isinstance(source, tuple) else source
                c = pltpu.make_async_copy(ref.at[at, span], ext.at[t, span], ext_sem.at[t])
                c.wait() if wait else c.start()

        if EDGE <= t < EDGE + LOCAL:
            copy(mine.at[0], t - EDGE, 1)
            return
        if t < EDGE:
            at, needed, crossed, refs = t, t >= EDGE - before, z == 0, (left, left_on)
        else:
            at, refs = t - EDGE - LOCAL, (right, right_on)
            needed, crossed = at < after, z == 3
        if wait:
            pl.when(needed)(lambda: copy(refs[0], at, 1))
        else:
            pl.when(needed & crossed)(lambda: copy(refs, at, 4))
            pl.when(needed & jnp.logical_not(crossed))(lambda: copy(refs[0], at, 1))

    @pl.when(u == 0)
    def _():
        row_copies(0, False)
        for t in range(2 * EDGE + LOCAL):
            tile_copies(t, False)
        for v in range(1, LOCAL):
            row_copies(v, False)

    row_copies(u, True)
    off[0, 0] = -rows[u].reshape(ANC * B, B)
    x = off[0, 0].T

    @pl.when(u == 0)
    def _():
        for t in range(2 * EDGE + LOCAL):
            tile_copies(t, True)

    first = u + EDGE - table[1, u]
    for j in range(0, LOCAL, 2):
        pair = jnp.concatenate([ext[first + j].reshape(ANC * B, B), ext[first + j + 1].reshape(ANC * B, B)], axis=1)
        inner = jnp.dot(x, pair, preferred_element_type=F32)
        for v in range(2):
            at = slice((j + v) * B, (j + v + 1) * B)
            kept = diag[0, 0, at].astype(F32) - inner[:, v * B:(v + 1) * B].T
            out[0, 0, at] = jnp.where(j + v < table[2, u], kept, 0.0).astype(BF16)


def on_device(sep_inv, panels, diag_inverse, widths, ancestors):
    steps = plan()
    sends = sum(s[0] == "send" for s in steps)
    any_space = pl.BlockSpec(memory_space=pl.ANY)
    smem = pl.BlockSpec(memory_space=pltpu.SMEM)
    dma = pltpu.SemaphoreType.DMA
    hbm = pl.BlockSpec(memory_space=pltpu.HBM)
    tiled = panels.reshape(1, LOCAL, ANC, B, B)
    ancestor_rows = ancestors.swapaxes(1, 2)
    table, spot = pl.pallas_call(
        table_kernel,
        name="table",
        in_specs=[smem, smem],
        out_specs=(smem, smem),
        out_shape=(jax.ShapeDtypeStruct((3, LOCAL), jnp.int32), jax.ShapeDtypeStruct((LOCAL, TILES), jnp.int32)),
    )(widths, ancestor_rows)
    y, left, right, left_on, right_on = pl.pallas_call(
        functools.partial(gather_kernel, steps),
        name="gather",
        out_shape=(
            jax.ShapeDtypeStruct((LOCAL, 8, 4, B, B), BF16),
        ) + (jax.ShapeDtypeStruct((EDGE, ANC, B, B), BF16),) * 4,
        in_specs=[any_space, any_space, smem],
        out_specs=(hbm,) * 5,
        scratch_shapes=[
            pltpu.VMEM((4, 4, 4, 4, B, KC), BF16),
            pltpu.VMEM((CHUNKS, KC, LOCAL * B), BF16),
            pltpu.VMEM((CHUNKS, KC, LOCAL * B), BF16),
            pltpu.VMEM((2, 6, 4, B, 256), F32),
            pltpu.VMEM((2, 6, B, 256), F32),
            pltpu.VMEM((LOCAL, 4, 4, B, B), BF16),
            pltpu.VMEM((LOCAL, 4, 4, B, B), BF16),
            pltpu.VMEM((LOCAL, ANC + 1, B, B), BF16),
            dma((4,)),
            dma,
            dma((sends,)),
            dma((sends,)),
            dma((SPREADS,)),
            dma((SPREADS,)),
            dma((12,)),
            dma((12,)),
            dma((12,)),
            dma((2,)),
            dma((2,)),
            dma((2, HALOS // 2)),
            dma((2, HALOS // 2)),
            dma((2, HALOS // 2)),
            dma((2, HALOS // 2)),
        ],
        compiler_params=pltpu.CompilerParams(
            collective_id=0, has_side_effects=True, vmem_limit_bytes=60 * 1024 * 1024
        ),
    )(sep_inv, tiled, spot)

    def unit(rows):
        return pl.BlockSpec((1, 1, rows, B), lambda u, *_: (0, u, 0, 0))

    off, diag = pl.pallas_call(
        finish_kernel,
        name="finish",
        grid_spec=pltpu.PrefetchScalarGridSpec(
            num_scalar_prefetch=2,
            grid=(LOCAL,),
            in_specs=[
                hbm, hbm, hbm, hbm, hbm, hbm, unit(LOCAL * B),
            ],
            out_specs=[unit(ANC * B), unit(LOCAL * B)],
            scratch_shapes=[
                pltpu.VMEM((2 * EDGE + LOCAL, ANC, B, B), BF16),
                pltpu.VMEM((LOCAL, ANC, B, B), BF16),
                dma((2 * EDGE + LOCAL,)),
                dma((LOCAL,)),
            ],
        ),
        out_shape=(
            jax.ShapeDtypeStruct((1, LOCAL, ANC * B, B), BF16),
            jax.ShapeDtypeStruct((1, LOCAL, LOCAL * B, B), BF16),
        ),
        compiler_params=pltpu.CompilerParams(vmem_limit_bytes=62 * 1024 * 1024),
    )(table, ancestor_rows, y.reshape(LOCAL, TILES, B, B), left, tiled, right, left_on, right_on, diag_inverse)
    return off, diag


def solution(mesh):
    placed = (
        P("grp", "dev"),
        P("grp", "dev", None, None),
        P("grp", "dev", None, None),
        P("grp", None),
        P("grp", None, None),
    )
    return jax.shard_map(
        on_device,
        mesh=mesh,
        in_specs=placed,
        out_specs=(P("grp", "dev", None, None), P("grp", "dev", None, None)),
        check_vma=False,
    )
```

```python
import functools
import heapq

import jax
import jax.numpy as jnp
from jax import lax
from jax.experimental import pallas as pl
from jax.experimental.pallas import tpu as pltpu
from jax.sharding import PartitionSpec as P

MESH = pl.DeviceIdType.MESH
F32 = jnp.float32
BF16 = jnp.bfloat16
PARTS = (
    (0, 0, 128, ("y", "z", "x")),
    (1, 0, 128, ("z", "y", "x")),
    (2, 0, 128, ("z", "x", "y")),
    (3, 0, 64, ("z", "x", "y")),
    (3, 64, 64, ("y", "x", "z")),
)
ORDER = tuple(p[3] for p in PARTS)
B = 128
LOCAL = 6
EDGE = 5
ANC = 16
TILES = 32
NSG = 32
CHUNKS = 16
KC = 256
SPREADS = 8
HALOS = 20
EDGES = (1, 3, 0, 5, 2, 7, 4, 9, 6, 11, 8, 13, 10, 15, 12, 17, 14, 19, 16, 18)


def plan():
    rate, latency, depth, edge = 42e3, 2.5, 4.0, 512 * B * 2
    steps, heap, got, held = [], [], {"edges": 0}, {2: [], 3: [], 4: []}
    queue = {(axis, s): [] for axis in ("x", "y", "z") for s in (1, -1)}
    free = {link: 0.0 for link in queue}
    tasks = [("spread", 0, i) for i in range(SPREADS)]
    clock = 0.0
    cost = {"spread": 0.5, "A": 1.25, "far": 0.95, "plane": 1.7, "group": 0.9}

    def send(m):
        part, phase, a, s, kind = m
        link = (ORDER[part][phase - 1], s)
        heapq.heappush(queue[link], (phase, kind == "half", len(steps), count("sent"), m))

    def pump():
        for link, waiting in queue.items():
            while waiting and free[link] < clock + depth:
                m = heapq.heappop(waiting)[4]
                size = PARTS[m[0]][2] * KC * 2 * (4 if m[1] == 3 else 1) // (2 if m[4] == "half" else 1)
                free[link] = max(clock, free[link]) + size / rate
                heapq.heappush(heap, (free[link] + latency, count("event"), m))
                steps.append(("send", m))
        while count("pump") and got["edges"] < HALOS and not queue["z", 1] and free["z", 1] < clock + depth:
            i = EDGES[got["edges"]]
            got["edges"] += 1
            for s in (1, -1):
                free["z", s] = max(clock, free["z", s]) + edge / rate
            steps.append(("edge", i))
            if i % 2:
                heapq.heappush(heap, (free["z", 1] + 2 * latency, count("event"), ("edge", i)))

    def near(part, phase, a):
        for s in (1, -1):
            send((part, phase, a, s, "near"))

    def count(key):
        got[key] = got.get(key, 0) + 1
        return got[key]

    def plane(part, rel):
        if part < 2:
            if count(("A", rel)) == 8:
                tasks.extend(("A", rel, i) for i in range(3))
        elif count((part, "plane", rel)) == 4:
            tasks.append(("plane", part, rel, count((part, "order"))))
            if got[(part, "order")] == 3:
                tasks.extend(held[part])

    def far(part, a):
        if part < 2:
            tasks.append(("far", part, a, count(("far", part))))
        else:
            group = ("group", part, a)
            (tasks if got.get((part, "order"), 0) == 3 else held[part]).append(group)

    def handle(m):
        part, phase, a, s, kind = m
        if phase == 1:
            if kind == "near":
                send((part, 1, 0, s, "half"))
                near(part, 2, -s)
                full = count((part, 1))
            elif count((part, 1, "far")) == 2:
                near(part, 2, 2)
                full = count((part, 1))
            else:
                full = 0
            if full == 3:
                near(part, 3, 0)
                plane(part, 0)
        elif phase == 2:
            if kind == "near":
                send((part, 2, a, s, "half"))
                if count((part, 2, -s)) == 4:
                    near(part, 3, -s)
                    plane(part, 0)
            elif count((part, 2, 2)) == 8:
                near(part, 3, 2)
                plane(part, 0)
        elif kind == "near":
            send((part, 3, a, s, "half"))
            plane(part, -s)
        elif count((part, 3, a, "far")) == 2:
            far(part, a)

    for phase in (1, 2):
        for part in range(len(PARTS)):
            near(part, phase, 0)
    pump()
    while heap or tasks or got["edges"] < HALOS:
        while heap and heap[0][0] <= clock:
            m = heapq.heappop(heap)[2]
            if m[0] == "edge":
                steps.append(("forward", m[1]))
                for s in (1, -1):
                    free["y", s] = max(clock, free["y", s]) + edge / rate
            else:
                steps.append(("wait", m))
                handle(m)
        pump()
        if tasks:
            task = tasks.pop(0)
            steps.append(("task",) + task)
            clock += cost[task[0]]
        elif heap:
            clock = max(clock, heap[0][0])
        else:
            clock += 1.0
    return steps


def spans(widths, position, table):
    def step(k, end):
        w = widths[0, k]

        @pl.when((end < position + LOCAL) & (end + w > position))
        def _():
            for u in range(LOCAL):
                @pl.when((position + u >= end) & (position + u < end + w))
                def _():
                    table[0, u] = k
                    table[1, u] = position + u - end
                    table[2, u] = w

        return end + w

    lax.fori_loop(0, NSG, step, jnp.int32(0))


def table_kernel(widths, ancestors, table, spot):
    spans(widths, lax.axis_index("dev") * LOCAL, table)
    for v in range(LOCAL):
        owner = table[0, v]
        for t in range(TILES):
            spot[v, t] = ANC
        for a in range(ANC):
            spot[v, ancestors[0, a, owner]] = a


def gather_kernel(
    steps, sep, panels, spot, y_out, left_out, right_out, left_on, right_on,
    blocks, own, other, total, last, stage_own, stage_other, pan,
    load_sem, pan_sem, send_sem, recv_sem, half_send, half_recv, y_local, y_send, y_recv, edge_send, edge_recv,
    hop_send, hop_recv, on_send, on_recv,
):
    grp, dev = lax.axis_index("grp"), lax.axis_index("dev")
    core = lax.rem(grp, 2)
    at = {"x": grp // 2, "y": dev // 4, "z": lax.rem(dev, 4)}

    def moved(axis, by):
        return lax.rem(at[axis] + by + 4, 4)

    def device(axis, by):
        to = dict(at)
        to[axis] = moved(axis, by)
        return (to["x"] * 2 + core, to["y"] * 4 + to["z"])

    partner = (at["x"] * 2 + 1 - core, dev)
    ahead, behind = (grp, lax.rem(dev + 1, 16)), (grp, lax.rem(dev + 15, 16))

    loads = [
        pltpu.make_async_copy(
            sep.at[pl.ds(p * B, B)], blocks.at[p, at["x"], at["y"], at["z"]], load_sem.at[p]
        )
        for p in range(4)
    ]
    pan_load = pltpu.make_async_copy(panels.at[0], pan.at[:, pl.ds(0, ANC)], pan_sem)
    for c in loads:
        c.start()
    pan_load.start()
    pan[:, ANC] = jnp.zeros((LOCAL, B, B), BF16)
    barrier = pltpu.get_barrier_semaphore()
    greeted = [device(a, s) for a in ("x", "y", "z") for s in (1, -1)] + [partner, ahead, behind]
    for d in greeted:
        pl.semaphore_signal(barrier, inc=1, device_id=d, device_id_type=MESH)
    for c in loads:
        c.wait()
    pl.semaphore_wait(barrier, len(greeted))

    number = {m: i for i, m in enumerate(s[1] for s in steps if s[0] == "send")}

    def message(m, arriving):
        part, phase, a, s, kind = m
        axes = ORDER[part]
        axis = axes[phase - 1]
        row, low, rows, _ = PARTS[part]
        where = dict(at)
        if phase == 2:
            where[axes[0]] = moved(axes[0], a)
        if phase == 3:
            where[axes[0]] = slice(None)
            where[axes[1]] = moved(axes[1], a)
        gone = (0 if kind == "near" else 1) + (1 if arriving else 0)
        where[axis] = moved(axis, -s * gone)
        columns = slice(None) if kind == "near" else pl.ds(0 if s == 1 else B, B)
        ref = blocks.at[row, where["x"], where["y"], where["z"], pl.ds(low, rows), columns]
        return pltpu.make_async_remote_copy(
            src_ref=ref, dst_ref=ref, send_sem=send_sem.at[number[m]], recv_sem=recv_sem.at[number[m]],
            device_id=device(axis, s), device_id_type=MESH,
        )

    def spread_copy(i):
        some = pl.ds(CHUNKS // SPREADS * i, CHUNKS // SPREADS)
        return pltpu.make_async_remote_copy(
            src_ref=own.at[some], dst_ref=other.at[some], send_sem=half_send.at[i], recv_sem=half_recv.at[i],
            device_id=partner, device_id_type=MESH,
        )

    def edge_copy(i):
        t, rows = i // 4, pl.ds((i % 4) * 4, 4)
        sides = ((panels.at[0, LOCAL - EDGE + t, rows], left_out, ahead, 1), (panels.at[0, t, rows], right_out, behind, -1))
        return [
            pltpu.make_async_remote_copy(
                src_ref=src, dst_ref=out.at[t, rows],
                send_sem=hop_send.at[e, i // 2] if i % 2 else edge_send.at[e],
                recv_sem=hop_recv.at[e, i // 2] if i % 2 else edge_recv.at[e],
                device_id=device("z", s) if i % 2 else d, device_id_type=MESH,
            )
            for e, (src, out, d, s) in enumerate(sides)
        ]

    def edge_on(i):
        t, rows = i // 4, pl.ds((i % 4) * 4, 4)
        return [
            pltpu.make_async_remote_copy(
                src_ref=out.at[t, rows], dst_ref=on.at[t, rows], send_sem=on_send.at[e, i // 2],
                recv_sem=on_recv.at[e, i // 2], device_id=device("y", s), device_id_type=MESH,
            )
            for e, (out, on, s) in enumerate(((left_out, left_on, 1), (right_out, right_on, -1)))
        ]

    last_dev = 15
    sends_edge, takes_edge = (dev < last_dev, dev > 0), (dev > 0, dev < last_dev)
    first_z, last_z = at["z"] == 0, at["z"] == 3
    sends_on = (first_z & (at["y"] < 3), last_z & (at["y"] > 0))
    takes_on = (first_z & (at["y"] > 0), last_z & (at["y"] < 3))

    def results(i, x, tiles):
        here, there = pl.ds(tiles, 2 if tiles == 0 else 1), 2 * x + core
        return (
            pltpu.make_async_copy(stage_own.at[:, x, here], y_out.at[:, there, here], y_local.at[i]),
            pltpu.make_async_remote_copy(
                src_ref=stage_other.at[:, x, here], dst_ref=y_out.at[:, there, here],
                send_sem=y_send.at[i], recv_sem=y_recv.at[i], device_id=partner, device_id_type=MESH,
            ),
        )

    def arrived(i, x, tiles):
        here, there = pl.ds(tiles, 2 if tiles == 0 else 1), 2 * x + 1 - core
        return pltpu.make_async_remote_copy(
            src_ref=y_out.at[:, there, here], dst_ref=y_out.at[:, there, here],
            send_sem=y_send.at[i], recv_sem=y_recv.at[i], device_id=partner, device_id_type=MESH,
        )

    queued = []

    def put(x, tiles):
        i = len(queued)
        queued.append((i, x, tiles))
        for c in results(i, x, tiles):
            c.start()

    sides = ((own, stage_own), (other, stage_other))

    def keep(stage, n, x, part, value):
        row, low, rows, _ = part
        for v in range(2):
            stage[2 * n + v, x, row, low:low + rows] = value[:, v * B:(v + 1) * B]

    def task_a(rel, n):
        x = moved("x", rel)
        cols = pl.ds(n * 256, 256)
        for source, stage in sides:
            acc = jnp.zeros((2 * B, 256), F32)
            for k in range(CHUNKS):
                lhs = blocks[0:2, x, k // 4, k % 4].reshape(2 * B, KC)
                acc = acc + jnp.dot(lhs, source[k, :, cols], preferred_element_type=F32)
            value = acc.astype(BF16)
            for p in range(2):
                keep(stage, n, x, PARTS[p], value[p * B:(p + 1) * B])

    def columns(body):
        def column(n, carry):
            for h, (source, stage) in enumerate(sides):
                body(n, pl.ds(pl.multiple_of(n * 256, 256), 256), 3 * h + n, source, stage)
            return carry

        lax.fori_loop(0, 3, column, 0)

    def task_far(part, a, nth):
        x, fixed = moved("x", 2), moved(ORDER[part][1], a)

        def body(n, cols, slot, source, stage):
            acc = jnp.zeros((B, 256), F32)
            for k in range(4):
                y, z = (k, fixed) if part == 0 else (fixed, k)
                acc = acc + jnp.dot(blocks[part, x, y, z], source[y * 4 + z, :, cols], preferred_element_type=F32)
            if nth > 1:
                acc = acc + last[part, slot]
            if nth < 4:
                last[part, slot] = acc
            else:
                keep(stage, n, x, PARTS[part], acc.astype(BF16))

        columns(body)

    def tile_of(part, fixed, k):
        return (fixed, k) if ORDER[part][2] == "y" else (k, fixed)

    def some(part):
        row, low, rows, _ = PARTS[part]
        return row, pl.ds(low, rows), rows

    def task_plane(part, rel, nth):
        row, span, rows = some(part)
        fixed = moved(ORDER[part][2], rel)

        def body(n, cols, slot, source, stage):
            acc = jnp.zeros((4 * rows, 256), F32)
            for k in range(4):
                y, z = tile_of(part, fixed, k)
                lhs = blocks[row, :, y, z, span].reshape(4 * rows, KC)
                acc = acc + jnp.dot(lhs, source[y * 4 + z, :, cols], preferred_element_type=F32)
            if nth > 1:
                acc = acc + total[row - 2, slot, :, span].reshape(4 * rows, 256)
            total[row - 2, slot, :, span] = acc.reshape(4, rows, 256)

        columns(body)

    def task_group(part, a):
        row, span, rows = some(part)
        fixed, x = moved(ORDER[part][2], 2), moved("x", a)

        def body(n, cols, slot, source, stage):
            acc = total[row - 2, slot, x, span]
            for k in range(4):
                y, z = tile_of(part, fixed, k)
                acc = acc + jnp.dot(blocks[row, x, y, z, span], source[y * 4 + z, :, cols], preferred_element_type=F32)
            keep(stage, n, x, PARTS[part], acc.astype(BF16))

        columns(body)

    def spread(i):
        for j in range(4):
            t = 4 * i + j
            for u in range(LOCAL):
                own[t // 2, (t % 2) * B:(t % 2 + 1) * B, u * B:(u + 1) * B] = pan[u, spot[u, t]]

    got_other, ended = False, {}
    for step in steps:
        if step[0] == "send":
            message(step[1], False).start()
        elif step[0] == "wait":
            message(step[1], True).wait_recv()
        elif step[0] == "edge":
            for c, sends in zip(edge_copy(step[1]), sends_edge):
                if step[1] % 2:
                    c.start()
                else:
                    pl.when(sends)(c.start)
        elif step[0] == "forward":
            for c in edge_copy(step[1]):
                c.wait_recv()
            for c, sends in zip(edge_on(step[1]), sends_on):
                pl.when(sends)(c.start)
        else:
            name = step[1]
            if name == "spread":
                i = step[3]
                if i == 0:
                    pan_load.wait()
                spread(i)
                if i > 0:
                    spread_copy(i - 1).start()
                continue
            if not got_other:
                spread_copy(SPREADS - 1).start()
                for j in range(SPREADS):
                    spread_copy(j).wait_recv()
                got_other = True
            if name == "A":
                task_a(step[2], step[3])
                if step[3] == 2:
                    put(moved("x", step[2]), 0)
            elif name == "far":
                task_far(*step[2:])
                ended["far"] = ended.get("far", 0) + 1
                if ended["far"] == 8:
                    put(moved("x", 2), 0)
            elif name == "plane":
                task_plane(*step[2:])
            else:
                task_group(*step[2:])
                key = (PARTS[step[2]][0], step[3])
                ended[key] = ended.get(key, 0) + PARTS[step[2]][2]
                if ended[key] == B:
                    put(moved("x", step[3]), key[0])

    for i, x, tiles in queued:
        arrived(i, x, tiles).wait_recv()
    for i, x, tiles in queued:
        local, remote = results(i, x, tiles)
        local.wait()
        remote.wait_send()
    for j in range(SPREADS):
        spread_copy(j).wait_send()
    for m in number:
        message(m, False).wait_send()
    for i in range(1, HALOS, 2):
        for c in edge_copy(i):
            c.wait_send()
        for c, sends, takes in zip(edge_on(i), sends_on, takes_on):
            pl.when(sends)(c.wait_send)
            pl.when(takes)(c.wait_recv)
    for e, (out, d) in enumerate(((left_out, ahead), (right_out, behind))):
        whole = pltpu.make_async_remote_copy(
            src_ref=panels.at[0, pl.ds(0, EDGE), pl.ds(0, ANC // 2)], dst_ref=out.at[:, pl.ds(0, ANC // 2)],
            send_sem=edge_send.at[e], recv_sem=edge_recv.at[e], device_id=d, device_id_type=MESH,
        )
        pl.when(takes_edge[e])(whole.wait_recv)
        pl.when(sends_edge[e])(whole.wait_send)


def finish_kernel(table, ancestors, y, left, mine, right, left_on, right_on, diag, off, out, ext, rows, ext_sem, row_sem):
    u = pl.program_id(0)
    z = lax.rem(lax.axis_index("dev"), 4)
    before, after = table[1, 0], table[2, LOCAL - 1] - 1 - table[1, LOCAL - 1]

    def row_copies(v, wait):
        if wait:
            pltpu.make_async_copy(y.at[v, pl.ds(0, ANC)], rows.at[v], row_sem.at[v]).wait()
        else:
            for a in range(ANC):
                pltpu.make_async_copy(
                    y.at[v, ancestors[0, a, table[0, v]]], rows.at[v, a], row_sem.at[v]
                ).start()

    def tile_copies(t, wait):
        def copy(source, at, parts):
            for q in range(0, ANC, ANC // parts):
                span = pl.ds(q, ANC // parts)
                ref = source[q // 4 % 2] if isinstance(source, tuple) else source
                c = pltpu.make_async_copy(ref.at[at, span], ext.at[t, span], ext_sem.at[t])
                c.wait() if wait else c.start()

        if EDGE <= t < EDGE + LOCAL:
            copy(mine.at[0], t - EDGE, 1)
            return
        if t < EDGE:
            at, needed, crossed, refs = t, t >= EDGE - before, z == 0, (left, left_on)
        else:
            at, refs = t - EDGE - LOCAL, (right, right_on)
            needed, crossed = at < after, z == 3
        if wait:
            pl.when(needed)(lambda: copy(refs[0], at, 1))
        else:
            pl.when(needed & crossed)(lambda: copy(refs, at, 4))
            pl.when(needed & jnp.logical_not(crossed))(lambda: copy(refs[0], at, 1))

    @pl.when(u == 0)
    def _():
        row_copies(0, False)
        for t in range(2 * EDGE + LOCAL):
            tile_copies(t, False)
        for v in range(1, LOCAL):
            row_copies(v, False)

    row_copies(u, True)
    off[0, 0] = -rows[u].reshape(ANC * B, B)
    x = off[0, 0].T

    @pl.when(u == 0)
    def _():
        for t in range(2 * EDGE + LOCAL):
            tile_copies(t, True)

    first = u + EDGE - table[1, u]
    for j in range(0, LOCAL, 2):
        pair = jnp.concatenate([ext[first + j].reshape(ANC * B, B), ext[first + j + 1].reshape(ANC * B, B)], axis=1)
        inner = jnp.dot(x, pair, preferred_element_type=F32)
        for v in range(2):
            at = slice((j + v) * B, (j + v + 1) * B)
            kept = diag[0, 0, at].astype(F32) - inner[:, v * B:(v + 1) * B].T
            out[0, 0, at] = jnp.where(j + v < table[2, u], kept, 0.0).astype(BF16)


def on_device(sep_inv, panels, diag_inverse, widths, ancestors):
    steps = plan()
    sends = sum(s[0] == "send" for s in steps)
    any_space = pl.BlockSpec(memory_space=pl.ANY)
    smem = pl.BlockSpec(memory_space=pltpu.SMEM)
    dma = pltpu.SemaphoreType.DMA
    hbm = pl.BlockSpec(memory_space=pltpu.HBM)
    tiled = panels.reshape(1, LOCAL, ANC, B, B)
    ancestor_rows = ancestors.swapaxes(1, 2)
    table, spot = pl.pallas_call(
        table_kernel,
        name="table",
        in_specs=[smem, smem],
        out_specs=(smem, smem),
        out_shape=(jax.ShapeDtypeStruct((3, LOCAL), jnp.int32), jax.ShapeDtypeStruct((LOCAL, TILES), jnp.int32)),
    )(widths, ancestor_rows)
    y, left, right, left_on, right_on = pl.pallas_call(
        functools.partial(gather_kernel, steps),
        name="gather",
        out_shape=(
            jax.ShapeDtypeStruct((LOCAL, 8, 4, B, B), BF16),
        ) + (jax.ShapeDtypeStruct((EDGE, ANC, B, B), BF16),) * 4,
        in_specs=[any_space, any_space, smem],
        out_specs=(hbm,) * 5,
        scratch_shapes=[
            pltpu.VMEM((4, 4, 4, 4, B, KC), BF16),
            pltpu.VMEM((CHUNKS, KC, LOCAL * B), BF16),
            pltpu.VMEM((CHUNKS, KC, LOCAL * B), BF16),
            pltpu.VMEM((2, 6, 4, B, 256), F32),
            pltpu.VMEM((2, 6, B, 256), F32),
            pltpu.VMEM((LOCAL, 4, 4, B, B), BF16),
            pltpu.VMEM((LOCAL, 4, 4, B, B), BF16),
            pltpu.VMEM((LOCAL, ANC + 1, B, B), BF16),
            dma((4,)),
            dma,
            dma((sends,)),
            dma((sends,)),
            dma((SPREADS,)),
            dma((SPREADS,)),
            dma((12,)),
            dma((12,)),
            dma((12,)),
            dma((2,)),
            dma((2,)),
            dma((2, HALOS // 2)),
            dma((2, HALOS // 2)),
            dma((2, HALOS // 2)),
            dma((2, HALOS // 2)),
        ],
        compiler_params=pltpu.CompilerParams(
            collective_id=0, has_side_effects=True, vmem_limit_bytes=60 * 1024 * 1024
        ),
    )(sep_inv, tiled, spot)

    def unit(rows):
        return pl.BlockSpec((1, 1, rows, B), lambda u, *_: (0, u, 0, 0))

    off, diag = pl.pallas_call(
        finish_kernel,
        name="finish",
        grid_spec=pltpu.PrefetchScalarGridSpec(
            num_scalar_prefetch=2,
            grid=(LOCAL,),
            in_specs=[
                hbm, hbm, hbm, hbm, hbm, hbm, unit(LOCAL * B),
            ],
            out_specs=[unit(ANC * B), unit(LOCAL * B)],
            scratch_shapes=[
                pltpu.VMEM((2 * EDGE + LOCAL, ANC, B, B), BF16),
                pltpu.VMEM((LOCAL, ANC, B, B), BF16),
                dma((2 * EDGE + LOCAL,)),
                dma((LOCAL,)),
            ],
        ),
        out_shape=(
            jax.ShapeDtypeStruct((1, LOCAL, ANC * B, B), BF16),
            jax.ShapeDtypeStruct((1, LOCAL, LOCAL * B, B), BF16),
        ),
        compiler_params=pltpu.CompilerParams(vmem_limit_bytes=62 * 1024 * 1024),
    )(table, ancestor_rows, y.reshape(LOCAL, TILES, B, B), left, tiled, right, left_on, right_on, diag_inverse)
    return off, diag


def solution(mesh):
    placed = (
        P("grp", "dev"),
        P("grp", "dev", None, None),
        P("grp", "dev", None, None),
        P("grp", None),
        P("grp", None, None),
    )
    return jax.shard_map(
        on_device,
        mesh=mesh,
        in_specs=placed,
        out_specs=(P("grp", "dev", None, None), P("grp", "dev", None, None)),
        check_vma=False,
    )
```

```python
import functools
import heapq

import jax
import jax.numpy as jnp
from jax import lax
from jax.experimental import pallas as pl
from jax.experimental.pallas import tpu as pltpu
from jax.sharding import PartitionSpec as P

MESH = pl.DeviceIdType.MESH
F32 = jnp.float32
BF16 = jnp.bfloat16
PARTS = (
    (0, 0, 128, ("y", "z", "x")),
    (1, 0, 128, ("z", "y", "x")),
    (2, 0, 128, ("z", "x", "y")),
    (3, 0, 64, ("z", "x", "y")),
    (3, 64, 64, ("y", "x", "z")),
)
ORDER = tuple(p[3] for p in PARTS)
B = 128
LOCAL = 6
EDGE = 5
ANC = 16
TILES = 32
NSG = 32
CHUNKS = 16
KC = 256
SPREADS = 8
HALOS = 20
EDGES = (1, 3, 0, 5, 2, 7, 4, 9, 6, 11, 8, 13, 10, 15, 12, 17, 14, 19, 16, 18)


def plan():
    rate, latency, depth, edge = 42e3, 2.5, 4.0, 512 * B * 2
    steps, heap, got, held = [], [], {"edges": 0}, {2: [], 3: [], 4: []}
    queue = {(axis, s): [] for axis in ("x", "y", "z") for s in (1, -1)}
    free = {link: 0.0 for link in queue}
    tasks = [("spread", 0, i) for i in range(SPREADS)]
    clock = 0.0
    cost = {"spread": 0.5, "A": 1.25, "far": 0.95, "plane": 1.7, "group": 0.9}

    def send(m):
        part, phase, a, s, kind = m
        link = (ORDER[part][phase - 1], s)
        heapq.heappush(queue[link], (phase, kind == "half", len(steps), count("sent"), m))

    def pump():
        for link, waiting in queue.items():
            while waiting and free[link] < clock + depth:
                m = heapq.heappop(waiting)[4]
                size = PARTS[m[0]][2] * KC * 2 * (4 if m[1] == 3 else 1) // (2 if m[4] == "half" else 1)
                free[link] = max(clock, free[link]) + size / rate
                heapq.heappush(heap, (free[link] + latency, count("event"), m))
                steps.append(("send", m))
        while count("pump") and got["edges"] < HALOS and not queue["z", 1] and free["z", 1] < clock + depth:
            i = EDGES[got["edges"]]
            got["edges"] += 1
            for s in (1, -1):
                free["z", s] = max(clock, free["z", s]) + edge / rate
            steps.append(("edge", i))
            if i % 2:
                heapq.heappush(heap, (free["z", 1] + 3 * latency, count("event"), ("edge", i)))

    def near(part, phase, a):
        for s in (1, -1):
            send((part, phase, a, s, "near"))

    def count(key):
        got[key] = got.get(key, 0) + 1
        return got[key]

    def plane(part, rel):
        if part < 2:
            if count(("A", rel)) == 8:
                tasks.extend(("A", rel, i) for i in range(3))
        elif count((part, "plane", rel)) == 4:
            tasks.append(("plane", part, rel, count((part, "order"))))
            if got[(part, "order")] == 3:
                tasks.extend(held[part])

    def far(part, a):
        if part < 2:
            tasks.append(("far", part, a, count(("far", part))))
        else:
            group = ("group", part, a)
            (tasks if got.get((part, "order"), 0) == 3 else held[part]).append(group)

    def handle(m):
        part, phase, a, s, kind = m
        if phase == 1:
            if kind == "near":
                send((part, 1, 0, s, "half"))
                near(part, 2, -s)
                full = count((part, 1))
            elif count((part, 1, "far")) == 2:
                near(part, 2, 2)
                full = count((part, 1))
            else:
                full = 0
            if full == 3:
                near(part, 3, 0)
                plane(part, 0)
        elif phase == 2:
            if kind == "near":
                send((part, 2, a, s, "half"))
                if count((part, 2, -s)) == 4:
                    near(part, 3, -s)
                    plane(part, 0)
            elif count((part, 2, 2)) == 8:
                near(part, 3, 2)
                plane(part, 0)
        elif kind == "near":
            send((part, 3, a, s, "half"))
            plane(part, -s)
        elif count((part, 3, a, "far")) == 2:
            far(part, a)

    for phase in (1, 2):
        for part in range(len(PARTS)):
            near(part, phase, 0)
    pump()
    while heap or tasks or got["edges"] < HALOS:
        while heap and heap[0][0] <= clock:
            m = heapq.heappop(heap)[2]
            if m[0] == "edge":
                steps.append(("forward", m[1]))
                for s in (1, -1):
                    free["y", s] = max(clock, free["y", s]) + edge / rate
            else:
                steps.append(("wait", m))
                handle(m)
        pump()
        if tasks:
            task = tasks.pop(0)
            steps.append(("task",) + task)
            clock += cost[task[0]]
        elif heap:
            clock = max(clock, heap[0][0])
        else:
            clock += 1.0
    return steps


def spans(widths, position, table):
    def step(k, end):
        w = widths[0, k]

        @pl.when((end < position + LOCAL) & (end + w > position))
        def _():
            for u in range(LOCAL):
                @pl.when((position + u >= end) & (position + u < end + w))
                def _():
                    table[0, u] = k
                    table[1, u] = position + u - end
                    table[2, u] = w

        return end + w

    lax.fori_loop(0, NSG, step, jnp.int32(0))


def table_kernel(widths, ancestors, table, spot):
    spans(widths, lax.axis_index("dev") * LOCAL, table)
    for v in range(LOCAL):
        owner = table[0, v]
        for t in range(TILES):
            spot[v, t] = ANC
        for a in range(ANC):
            spot[v, ancestors[0, a, owner]] = a


def gather_kernel(
    steps, sep, panels, spot, y_out, left_out, right_out, left_on, right_on,
    blocks, own, other, total, last, stage_own, stage_other, pan,
    load_sem, pan_sem, send_sem, recv_sem, half_send, half_recv, y_local, y_send, y_recv, edge_send, edge_recv,
    hop_send, hop_recv, on_send, on_recv,
):
    grp, dev = lax.axis_index("grp"), lax.axis_index("dev")
    core = lax.rem(grp, 2)
    at = {"x": grp // 2, "y": dev // 4, "z": lax.rem(dev, 4)}

    def moved(axis, by):
        return lax.rem(at[axis] + by + 4, 4)

    def device(axis, by):
        to = dict(at)
        to[axis] = moved(axis, by)
        return (to["x"] * 2 + core, to["y"] * 4 + to["z"])

    partner = (at["x"] * 2 + 1 - core, dev)
    ahead, behind = (grp, lax.rem(dev + 1, 16)), (grp, lax.rem(dev + 15, 16))

    loads = [
        pltpu.make_async_copy(
            sep.at[pl.ds(p * B, B)], blocks.at[p, at["x"], at["y"], at["z"]], load_sem.at[p]
        )
        for p in range(4)
    ]
    pan_load = pltpu.make_async_copy(panels.at[0], pan.at[:, pl.ds(0, ANC)], pan_sem)
    for c in loads:
        c.start()
    pan_load.start()
    pan[:, ANC] = jnp.zeros((LOCAL, B, B), BF16)
    barrier = pltpu.get_barrier_semaphore()
    greeted = [device(a, s) for a in ("x", "y", "z") for s in (1, -1)] + [partner, ahead, behind]
    for d in greeted:
        pl.semaphore_signal(barrier, inc=1, device_id=d, device_id_type=MESH)
    for c in loads:
        c.wait()
    pl.semaphore_wait(barrier, len(greeted))

    number = {m: i for i, m in enumerate(s[1] for s in steps if s[0] == "send")}

    def message(m, arriving):
        part, phase, a, s, kind = m
        axes = ORDER[part]
        axis = axes[phase - 1]
        row, low, rows, _ = PARTS[part]
        where = dict(at)
        if phase == 2:
            where[axes[0]] = moved(axes[0], a)
        if phase == 3:
            where[axes[0]] = slice(None)
            where[axes[1]] = moved(axes[1], a)
        gone = (0 if kind == "near" else 1) + (1 if arriving else 0)
        where[axis] = moved(axis, -s * gone)
        columns = slice(None) if kind == "near" else pl.ds(0 if s == 1 else B, B)
        ref = blocks.at[row, where["x"], where["y"], where["z"], pl.ds(low, rows), columns]
        return pltpu.make_async_remote_copy(
            src_ref=ref, dst_ref=ref, send_sem=send_sem.at[number[m]], recv_sem=recv_sem.at[number[m]],
            device_id=device(axis, s), device_id_type=MESH,
        )

    def spread_copy(i):
        some = pl.ds(CHUNKS // SPREADS * i, CHUNKS // SPREADS)
        return pltpu.make_async_remote_copy(
            src_ref=own.at[some], dst_ref=other.at[some], send_sem=half_send.at[i], recv_sem=half_recv.at[i],
            device_id=partner, device_id_type=MESH,
        )

    def edge_copy(i):
        t, rows = i // 4, pl.ds((i % 4) * 4, 4)
        sides = ((panels.at[0, LOCAL - EDGE + t, rows], left_out, ahead, 1), (panels.at[0, t, rows], right_out, behind, -1))
        return [
            pltpu.make_async_remote_copy(
                src_ref=src, dst_ref=out.at[t, rows],
                send_sem=hop_send.at[e, i // 2] if i % 2 else edge_send.at[e],
                recv_sem=hop_recv.at[e, i // 2] if i % 2 else edge_recv.at[e],
                device_id=device("z", s) if i % 2 else d, device_id_type=MESH,
            )
            for e, (src, out, d, s) in enumerate(sides)
        ]

    def edge_on(i):
        t, rows = i // 4, pl.ds((i % 4) * 4, 4)
        return [
            pltpu.make_async_remote_copy(
                src_ref=out.at[t, rows], dst_ref=on.at[t, rows], send_sem=on_send.at[e, i // 2],
                recv_sem=on_recv.at[e, i // 2], device_id=device("y", s), device_id_type=MESH,
            )
            for e, (out, on, s) in enumerate(((left_out, left_on, 1), (right_out, right_on, -1)))
        ]

    last_dev = 15
    sends_edge, takes_edge = (dev < last_dev, dev > 0), (dev > 0, dev < last_dev)
    first_z, last_z = at["z"] == 0, at["z"] == 3
    sends_on = (first_z & (at["y"] < 3), last_z & (at["y"] > 0))
    takes_on = (first_z & (at["y"] > 0), last_z & (at["y"] < 3))

    def results(i, x, tiles):
        here, there = pl.ds(tiles, 2 if tiles == 0 else 1), 2 * x + core
        return (
            pltpu.make_async_copy(stage_own.at[:, x, here], y_out.at[:, there, here], y_local.at[i]),
            pltpu.make_async_remote_copy(
                src_ref=stage_other.at[:, x, here], dst_ref=y_out.at[:, there, here],
                send_sem=y_send.at[i], recv_sem=y_recv.at[i], device_id=partner, device_id_type=MESH,
            ),
        )

    def arrived(i, x, tiles):
        here, there = pl.ds(tiles, 2 if tiles == 0 else 1), 2 * x + 1 - core
        return pltpu.make_async_remote_copy(
            src_ref=y_out.at[:, there, here], dst_ref=y_out.at[:, there, here],
            send_sem=y_send.at[i], recv_sem=y_recv.at[i], device_id=partner, device_id_type=MESH,
        )

    queued = []

    def put(x, tiles):
        i = len(queued)
        queued.append((i, x, tiles))
        for c in results(i, x, tiles):
            c.start()

    sides = ((own, stage_own), (other, stage_other))

    def keep(stage, n, x, part, value):
        row, low, rows, _ = part
        for v in range(2):
            stage[2 * n + v, x, row, low:low + rows] = value[:, v * B:(v + 1) * B]

    def task_a(rel, n):
        x = moved("x", rel)
        cols = pl.ds(n * 256, 256)
        for source, stage in sides:
            acc = jnp.zeros((2 * B, 256), F32)
            for k in range(CHUNKS):
                lhs = blocks[0:2, x, k // 4, k % 4].reshape(2 * B, KC)
                acc = acc + jnp.dot(lhs, source[k, :, cols], preferred_element_type=F32)
            value = acc.astype(BF16)
            for p in range(2):
                keep(stage, n, x, PARTS[p], value[p * B:(p + 1) * B])

    def columns(body):
        def column(n, carry):
            for h, (source, stage) in enumerate(sides):
                body(n, pl.ds(pl.multiple_of(n * 256, 256), 256), 3 * h + n, source, stage)
            return carry

        lax.fori_loop(0, 3, column, 0)

    def task_far(part, a, nth):
        x, fixed = moved("x", 2), moved(ORDER[part][1], a)

        def body(n, cols, slot, source, stage):
            acc = jnp.zeros((B, 256), F32)
            for k in range(4):
                y, z = (k, fixed) if part == 0 else (fixed, k)
                acc = acc + jnp.dot(blocks[part, x, y, z], source[y * 4 + z, :, cols], preferred_element_type=F32)
            if nth > 1:
                acc = acc + last[part, slot]
            if nth < 4:
                last[part, slot] = acc
            else:
                keep(stage, n, x, PARTS[part], acc.astype(BF16))

        columns(body)

    def tile_of(part, fixed, k):
        return (fixed, k) if ORDER[part][2] == "y" else (k, fixed)

    def some(part):
        row, low, rows, _ = PARTS[part]
        return row, pl.ds(low, rows), rows

    def task_plane(part, rel, nth):
        row, span, rows = some(part)
        fixed = moved(ORDER[part][2], rel)

        def body(n, cols, slot, source, stage):
            acc = jnp.zeros((4 * rows, 256), F32)
            for k in range(4):
                y, z = tile_of(part, fixed, k)
                lhs = blocks[row, :, y, z, span].reshape(4 * rows, KC)
                acc = acc + jnp.dot(lhs, source[y * 4 + z, :, cols], preferred_element_type=F32)
            if nth > 1:
                acc = acc + total[row - 2, slot, :, span].reshape(4 * rows, 256)
            total[row - 2, slot, :, span] = acc.reshape(4, rows, 256)

        columns(body)

    def task_group(part, a):
        row, span, rows = some(part)
        fixed, x = moved(ORDER[part][2], 2), moved("x", a)

        def body(n, cols, slot, source, stage):
            acc = total[row - 2, slot, x, span]
            for k in range(4):
                y, z = tile_of(part, fixed, k)
                acc = acc + jnp.dot(blocks[row, x, y, z, span], source[y * 4 + z, :, cols], preferred_element_type=F32)
            keep(stage, n, x, PARTS[part], acc.astype(BF16))

        columns(body)

    def spread(i):
        for j in range(4):
            t = 4 * i + j
            for u in range(LOCAL):
                own[t // 2, (t % 2) * B:(t % 2 + 1) * B, u * B:(u + 1) * B] = pan[u, spot[u, t]]

    got_other, ended = False, {}
    for step in steps:
        if step[0] == "send":
            message(step[1], False).start()
        elif step[0] == "wait":
            message(step[1], True).wait_recv()
        elif step[0] == "edge":
            for c, sends in zip(edge_copy(step[1]), sends_edge):
                if step[1] % 2:
                    c.start()
                else:
                    pl.when(sends)(c.start)
        elif step[0] == "forward":
            for c in edge_copy(step[1]):
                c.wait_recv()
            for c, sends in zip(edge_on(step[1]), sends_on):
                pl.when(sends)(c.start)
        else:
            name = step[1]
            if name == "spread":
                i = step[3]
                if i == 0:
                    pan_load.wait()
                spread(i)
                if i > 0:
                    spread_copy(i - 1).start()
                continue
            if not got_other:
                spread_copy(SPREADS - 1).start()
                for j in range(SPREADS):
                    spread_copy(j).wait_recv()
                got_other = True
            if name == "A":
                task_a(step[2], step[3])
                if step[3] == 2:
                    put(moved("x", step[2]), 0)
            elif name == "far":
                task_far(*step[2:])
                ended["far"] = ended.get("far", 0) + 1
                if ended["far"] == 8:
                    put(moved("x", 2), 0)
            elif name == "plane":
                task_plane(*step[2:])
            else:
                task_group(*step[2:])
                key = (PARTS[step[2]][0], step[3])
                ended[key] = ended.get(key, 0) + PARTS[step[2]][2]
                if ended[key] == B:
                    put(moved("x", step[3]), key[0])

    for i, x, tiles in queued:
        arrived(i, x, tiles).wait_recv()
    for i, x, tiles in queued:
        local, remote = results(i, x, tiles)
        local.wait()
        remote.wait_send()
    for j in range(SPREADS):
        spread_copy(j).wait_send()
    for m in number:
        message(m, False).wait_send()
    for i in range(1, HALOS, 2):
        for c in edge_copy(i):
            c.wait_send()
        for c, sends, takes in zip(edge_on(i), sends_on, takes_on):
            pl.when(sends)(c.wait_send)
            pl.when(takes)(c.wait_recv)
    for e, (out, d) in enumerate(((left_out, ahead), (right_out, behind))):
        whole = pltpu.make_async_remote_copy(
            src_ref=panels.at[0, pl.ds(0, EDGE), pl.ds(0, ANC // 2)], dst_ref=out.at[:, pl.ds(0, ANC // 2)],
            send_sem=edge_send.at[e], recv_sem=edge_recv.at[e], device_id=d, device_id_type=MESH,
        )
        pl.when(takes_edge[e])(whole.wait_recv)
        pl.when(sends_edge[e])(whole.wait_send)


def finish_kernel(table, ancestors, y, left, mine, right, left_on, right_on, diag, off, out, ext, rows, ext_sem, row_sem):
    u = pl.program_id(0)
    z = lax.rem(lax.axis_index("dev"), 4)
    before, after = table[1, 0], table[2, LOCAL - 1] - 1 - table[1, LOCAL - 1]

    def row_copies(v, wait):
        if wait:
            pltpu.make_async_copy(y.at[v, pl.ds(0, ANC)], rows.at[v], row_sem.at[v]).wait()
        else:
            for a in range(ANC):
                pltpu.make_async_copy(
                    y.at[v, ancestors[0, a, table[0, v]]], rows.at[v, a], row_sem.at[v]
                ).start()

    def tile_copies(t, wait):
        def copy(source, at, parts):
            for q in range(0, ANC, ANC // parts):
                span = pl.ds(q, ANC // parts)
                ref = source[q // 4 % 2] if isinstance(source, tuple) else source
                c = pltpu.make_async_copy(ref.at[at, span], ext.at[t, span], ext_sem.at[t])
                c.wait() if wait else c.start()

        if EDGE <= t < EDGE + LOCAL:
            copy(mine.at[0], t - EDGE, 1)
            return
        if t < EDGE:
            at, needed, crossed, refs = t, t >= EDGE - before, z == 0, (left, left_on)
        else:
            at, refs = t - EDGE - LOCAL, (right, right_on)
            needed, crossed = at < after, z == 3
        if wait:
            pl.when(needed)(lambda: copy(refs[0], at, 1))
        else:
            pl.when(needed & crossed)(lambda: copy(refs, at, 4))
            pl.when(needed & jnp.logical_not(crossed))(lambda: copy(refs[0], at, 1))

    @pl.when(u == 0)
    def _():
        row_copies(0, False)
        for t in range(2 * EDGE + LOCAL):
            tile_copies(t, False)
        for v in range(1, LOCAL):
            row_copies(v, False)

    row_copies(u, True)
    off[0, 0] = -rows[u].reshape(ANC * B, B)
    x = off[0, 0].T

    @pl.when(u == 0)
    def _():
        for t in range(2 * EDGE + LOCAL):
            tile_copies(t, True)

    first = u + EDGE - table[1, u]
    for j in range(0, LOCAL, 2):
        pair = jnp.concatenate([ext[first + j].reshape(ANC * B, B), ext[first + j + 1].reshape(ANC * B, B)], axis=1)
        inner = jnp.dot(x, pair, preferred_element_type=F32)
        for v in range(2):
            at = slice((j + v) * B, (j + v + 1) * B)
            kept = diag[0, 0, at].astype(F32) - inner[:, v * B:(v + 1) * B].T
            out[0, 0, at] = jnp.where(j + v < table[2, u], kept, 0.0).astype(BF16)


def on_device(sep_inv, panels, diag_inverse, widths, ancestors):
    steps = plan()
    sends = sum(s[0] == "send" for s in steps)
    any_space = pl.BlockSpec(memory_space=pl.ANY)
    smem = pl.BlockSpec(memory_space=pltpu.SMEM)
    dma = pltpu.SemaphoreType.DMA
    hbm = pl.BlockSpec(memory_space=pltpu.HBM)
    tiled = panels.reshape(1, LOCAL, ANC, B, B)
    ancestor_rows = ancestors.swapaxes(1, 2)
    table, spot = pl.pallas_call(
        table_kernel,
        name="table",
        in_specs=[smem, smem],
        out_specs=(smem, smem),
        out_shape=(jax.ShapeDtypeStruct((3, LOCAL), jnp.int32), jax.ShapeDtypeStruct((LOCAL, TILES), jnp.int32)),
    )(widths, ancestor_rows)
    y, left, right, left_on, right_on = pl.pallas_call(
        functools.partial(gather_kernel, steps),
        name="gather",
        out_shape=(
            jax.ShapeDtypeStruct((LOCAL, 8, 4, B, B), BF16),
        ) + (jax.ShapeDtypeStruct((EDGE, ANC, B, B), BF16),) * 4,
        in_specs=[any_space, any_space, smem],
        out_specs=(hbm,) * 5,
        scratch_shapes=[
            pltpu.VMEM((4, 4, 4, 4, B, KC), BF16),
            pltpu.VMEM((CHUNKS, KC, LOCAL * B), BF16),
            pltpu.VMEM((CHUNKS, KC, LOCAL * B), BF16),
            pltpu.VMEM((2, 6, 4, B, 256), F32),
            pltpu.VMEM((2, 6, B, 256), F32),
            pltpu.VMEM((LOCAL, 4, 4, B, B), BF16),
            pltpu.VMEM((LOCAL, 4, 4, B, B), BF16),
            pltpu.VMEM((LOCAL, ANC + 1, B, B), BF16),
            dma((4,)),
            dma,
            dma((sends,)),
            dma((sends,)),
            dma((SPREADS,)),
            dma((SPREADS,)),
            dma((12,)),
            dma((12,)),
            dma((12,)),
            dma((2,)),
            dma((2,)),
            dma((2, HALOS // 2)),
            dma((2, HALOS // 2)),
            dma((2, HALOS // 2)),
            dma((2, HALOS // 2)),
        ],
        compiler_params=pltpu.CompilerParams(
            collective_id=0, has_side_effects=True, vmem_limit_bytes=60 * 1024 * 1024
        ),
    )(sep_inv, tiled, spot)

    def unit(rows):
        return pl.BlockSpec((1, 1, rows, B), lambda u, *_: (0, u, 0, 0))

    off, diag = pl.pallas_call(
        finish_kernel,
        name="finish",
        grid_spec=pltpu.PrefetchScalarGridSpec(
            num_scalar_prefetch=2,
            grid=(LOCAL,),
            in_specs=[
                hbm, hbm, hbm, hbm, hbm, hbm, unit(LOCAL * B),
            ],
            out_specs=[unit(ANC * B), unit(LOCAL * B)],
            scratch_shapes=[
                pltpu.VMEM((2 * EDGE + LOCAL, ANC, B, B), BF16),
                pltpu.VMEM((LOCAL, ANC, B, B), BF16),
                dma((2 * EDGE + LOCAL,)),
                dma((LOCAL,)),
            ],
        ),
        out_shape=(
            jax.ShapeDtypeStruct((1, LOCAL, ANC * B, B), BF16),
            jax.ShapeDtypeStruct((1, LOCAL, LOCAL * B, B), BF16),
        ),
        compiler_params=pltpu.CompilerParams(vmem_limit_bytes=62 * 1024 * 1024),
    )(table, ancestor_rows, y.reshape(LOCAL, TILES, B, B), left, tiled, right, left_on, right_on, diag_inverse)
    return off, diag


def solution(mesh):
    placed = (
        P("grp", "dev"),
        P("grp", "dev", None, None),
        P("grp", "dev", None, None),
        P("grp", None),
        P("grp", None, None),
    )
    return jax.shard_map(
        on_device,
        mesh=mesh,
        in_specs=placed,
        out_specs=(P("grp", "dev", None, None), P("grp", "dev", None, None)),
        check_vma=False,
    )
```
